32 devices in a mesh: gx: 8 (over y, x, core), yz: 4 (over z).
Axes of the slice: x: 2, y: 2, z: 4, core: 2. Of those that a mesh axis runs over, the one named last changes fastest.
Arguments:
- vel: float32 [3, 48, 192, 1024], P(None, 'gx', 'yz'), may hold values from -6 to 6
- q_old: float32 [3, 48, 192, 1024], P(None, 'gx', None, 'yz'), may hold values from -6 to 6
- pressure_guess: float32 [48, 192, 1024], P('gx', None, 'yz'), may hold values from -6 to 6
- shear_shift: int32 [1], replicated, may hold values from 0 to 1023
Outputs:
- vel_next: float32 [3, 48, 192, 1024], P(None, 'gx', 'yz')
- q_next: float32 [3, 48, 192, 1024], P(None, 'gx', None, 'yz')
- pressure: float32 [48, 192, 1024], P('gx', None, 'yz')
The draws below stay inside these ranges and needn't reach their ends.
All inputs are finite; a program needn't handle non-finite values.
Results may differ from the reference program's by a relative error of at most 0.00013.
Values sent between devices are 32-bit elements; how exact they have to be, the bound alone decides.
No kernel may reach another device: no remote copies, remote signals or barrier semaphores. Data moves between devices by JAX's collectives and lax.ppermute only.
A program may use at most 128 MiB of HBM per device.

```python
import math
import jax
import jax.numpy as jnp
from jax import lax

NY = 1024
NZ = 192
SWEEPS = 2
NX = 48
N_YZ = 4


def steps_of(rng, dims, cuts, smallest, top_value):
    def one(axis_at, shards_of):
        heights = jax.random.uniform(jax.random.fold_in(jax.random.fold_in(rng, 6), axis_at), (shards_of,), jnp.float32, smallest / len(cuts), top_value / len(cuts))
        return jnp.repeat(jnp.exp(heights), dims[axis_at] // shards_of).reshape((-1,) + (1,) * (len(dims) - axis_at - 1))

    factor_of = one(*cuts[0])
    for cut in cuts[1:]:
        factor_of = factor_of * one(*cut)
    return factor_of


def noise(key, extent, spread, bound, shards=(), kind=jnp.bfloat16):
    array = spread * jax.random.normal(key, extent, jnp.float32)
    if shards:
        array = array * steps_of(key, extent, shards, -0.22, 0.18)
    return jnp.clip(array, -bound, bound).astype(kind)


def setup_inputs(seed: int = 0) -> dict:
    streams_of = jax.random.split(jax.random.key(seed), 5)
    return {
        "vel": noise(streams_of[0], (3, NX, NZ, NY), 1.0, 6.0, ((1, 8), (2, 4)), jnp.float32),
        "q_old": noise(streams_of[1], (3, NX, NZ, NY), 1.0, 6.0, ((1, 8), (3, 4)), jnp.float32),
        "pressure_guess": noise(streams_of[2], (NX, NZ, NY), 1.0, 6.0, ((0, 8), (2, 4)), jnp.float32),
        "shear_shift": jax.random.randint(streams_of[3], (1,), 0, NY).astype(jnp.int32),
    }


highest = lax.Precision.HIGHEST
viscosity = 0.05
time_step = 0.2
keep_weight = -5.0 / 9.0
section_weight = 15.0 / 16.0
shear_param = 1.5
fraction = 0.375

def unpack(packed):
    leading = packed.shape[:-1]
    block_len = NY // (2 * N_YZ)
    viewed = packed.reshape(leading + (N_YZ, 2, block_len))
    return (viewed[..., 0, :].reshape(leading + (NY // 2,)), viewed[..., 1, :].reshape(leading + (NY // 2,)))

def pack(real_part, imag_part):
    leading = real_part.shape[:-1]
    block_len = NY // (2 * N_YZ)
    viewed = jnp.stack([real_part.reshape(leading + (N_YZ, block_len)), imag_part.reshape(leading + (N_YZ, block_len))], axis=-2)
    return viewed.reshape(leading + (NY,))

def x_slice(padded, offset):
    return padded[:, 3 + offset:3 + offset + NX]

def first_diff(padded):
    return (45.0 * (x_slice(padded, 1) - x_slice(padded, -1)) - 9.0 * (x_slice(padded, 2) - x_slice(padded, -2)) + (x_slice(padded, 3) - x_slice(padded, -3))) / 60.0

def second_diff(padded):
    return (2.0 * (x_slice(padded, 3) + x_slice(padded, -3)) - 27.0 * (x_slice(padded, 2) + x_slice(padded, -2)) + 270.0 * (x_slice(padded, 1) + x_slice(padded, -1)) - 490.0 * x_slice(padded, 0)) / 180.0

def rotate(real_part, imag_part, cosine, sine):
    return (real_part * cosine - imag_part * sine, real_part * sine + imag_part * cosine)

def reference(vel, q_old, pressure_guess, shear_shift):
    offset = shear_shift[0]
    tail_rows = vel[:, NX - 3:]
    front_rows = vel[:, :3]
    left_rim = (1.0 - fraction) * jnp.roll(tail_rows, -offset, axis=3) + fraction * jnp.roll(tail_rows, -offset - 1, axis=3)
    right_rim = (1.0 - fraction) * jnp.roll(front_rows, offset, axis=3) + fraction * jnp.roll(front_rows, offset + 1, axis=3)
    padded = jnp.concatenate([left_rim, vel, right_rim], axis=1)
    omega = 2.0 / NX
    xpos = jnp.arange(NX, dtype=jnp.int32).astype(jnp.float32) + 0.5 - NX / 2.0
    background = (-shear_param * omega * xpos)[:, None, None]
    coriolis = jnp.stack([2.0 * omega * vel[1], -(2.0 - shear_param) * omega * vel[0], jnp.zeros_like(vel[0])])
    term_a = -first_diff(padded * padded[0][None]) + viscosity * second_diff(padded) + coriolis
    term_b = -(vel[1] + background)[None] * vel
    term_c = -vel[2][None] * vel
    modes = jnp.arange(NY // 2, dtype=jnp.int32)
    cells_y = jnp.arange(NY, dtype=jnp.int32)
    angle_y = 2.0 * math.pi / NY * (cells_y[:, None] * modes[None, :] % NY).astype(jnp.float32)
    cos_y = jnp.cos(angle_y) / math.sqrt(NY)
    sin_y = jnp.sin(angle_y) / math.sqrt(NY)

    def y_forward(field):
        return (jnp.einsum('cxzy,yk->cxzk', field, cos_y, precision=highest), -jnp.einsum('cxzy,yk->cxzk', field, sin_y, precision=highest))
    ya_re, ya_im = y_forward(term_a)
    yb_re, yb_im = y_forward(term_b)
    yc_re, yc_im = y_forward(term_c)
    yu_re, yu_im = y_forward(vel)
    wave_y = 2.0 * math.pi / NY * modes.astype(jnp.float32)
    w_re = ya_re - wave_y * yb_im - viscosity * (wave_y * wave_y) * yu_re
    w_im = ya_im + wave_y * yb_re - viscosity * (wave_y * wave_y) * yu_im
    cells_z = jnp.arange(NZ, dtype=jnp.int32)
    angle_z = 2.0 * math.pi / NZ * (cells_z[:, None] * cells_z[None, :] % NZ).astype(jnp.float32)
    cos_z = jnp.cos(angle_z) / math.sqrt(NZ)
    sin_z = jnp.sin(angle_z) / math.sqrt(NZ)
    signed_z = jnp.where(cells_z < NZ // 2, cells_z, cells_z - NZ)
    wave_z = (2.0 * math.pi / NZ * signed_z.astype(jnp.float32))[:, None]

    def z_apply(real_part, imag_part, sign):
        cos_re = jnp.einsum('wz,cxzk->cxwk', cos_z, real_part, precision=highest)
        cos_im = jnp.einsum('wz,cxzk->cxwk', cos_z, imag_part, precision=highest)
        sin_re = jnp.einsum('wz,cxzk->cxwk', sin_z, real_part, precision=highest)
        sin_im = jnp.einsum('wz,cxzk->cxwk', sin_z, imag_part, precision=highest)
        return (cos_re + sign * sin_im, cos_im - sign * sin_re)
    zw_re, zw_im = z_apply(w_re, w_im, 1.0)
    zc_re, zc_im = z_apply(yc_re, yc_im, 1.0)
    zu_re, zu_im = z_apply(yu_re, yu_im, 1.0)
    tend_re = zw_re - wave_z * zc_im - viscosity * (wave_z * wave_z) * zu_re
    tend_im = zw_im + wave_z * zc_re - viscosity * (wave_z * wave_z) * zu_im
    edge_angle = 2.0 * math.pi / NY * ((modes * offset % NY).astype(jnp.float32) + fraction * modes.astype(jnp.float32))
    edge_cos = jnp.cos(edge_angle)
    edge_sin = jnp.sin(edge_angle)

    def neighbours(real_part, imag_part):
        low_re, low_im = rotate(real_part[NX - 1:], imag_part[NX - 1:], edge_cos, edge_sin)
        high_re, high_im = rotate(real_part[:1], imag_part[:1], edge_cos, -edge_sin)
        plus_re = jnp.concatenate([real_part[1:], high_re], axis=0)
        plus_im = jnp.concatenate([imag_part[1:], high_im], axis=0)
        minus_re = jnp.concatenate([low_re, real_part[:-1]], axis=0)
        minus_im = jnp.concatenate([low_im, imag_part[:-1]], axis=0)
        return (plus_re, plus_im, minus_re, minus_im)
    xp_re, xp_im, xm_re, xm_im = neighbours(tend_re[0], tend_im[0])
    div_re = 0.5 * (xp_re - xm_re) - wave_y * tend_im[1] - wave_z * tend_im[2]
    div_im = 0.5 * (xp_im - xm_im) + wave_y * tend_re[1] + wave_z * tend_re[2]
    denom = 2.0 + wave_y[None, :] * wave_y[None, :] + wave_z * wave_z
    press_re, press_im = unpack(pressure_guess)
    for sweep_no in range(SWEEPS):
        pp_re, pp_im, pm_re, pm_im = neighbours(press_re, press_im)
        press_re = (pp_re + pm_re - div_re) / denom
        press_im = (pp_im + pm_im - div_im) / denom
    pp_re, pp_im, pm_re, pm_im = neighbours(press_re, press_im)
    grad_re = jnp.stack([0.5 * (pp_re - pm_re), -wave_y * press_im, -wave_z * press_im])
    grad_im = jnp.stack([0.5 * (pp_im - pm_im), wave_y * press_re, wave_z * press_re])
    old_re, old_im = unpack(q_old)
    new_re = keep_weight * old_re + time_step * (tend_re - grad_re)
    new_im = keep_weight * old_im + time_step * (tend_im - grad_im)
    q_next = pack(new_re, new_im)
    back_re, back_im = z_apply(new_re, new_im, -1.0)
    weights = jnp.where(modes == 0, 1.0, 2.0).astype(jnp.float32)
    correction = jnp.einsum('cxzk,yk->cxzy', back_re, cos_y * weights[None, :], precision=highest) - jnp.einsum('cxzk,yk->cxzy', back_im, sin_y * weights[None, :], precision=highest)
    vel_next = vel + section_weight * correction
    return (vel_next, q_next, pack(press_re, press_im))
```

```python
import math

import jax
import jax.numpy as jnp
from jax import lax
from jax.experimental import pallas as pl
from jax.experimental.pallas import tpu as pltpu
from jax.sharding import PartitionSpec as P

SWEEPS = 2
viscosity = 0.05
time_step = 0.2
keep_weight = -5.0 / 9.0
section_weight = 15.0 / 16.0
shear_param = 1.5
fraction = 0.375
f32 = jnp.float32
bf16 = jnp.bfloat16
VMEM_BYTES = 60 * 1024 * 1024


def params(n=1):
    return pltpu.CompilerParams(
        vmem_limit_bytes=VMEM_BYTES, dimension_semantics=("arbitrary",) * n
    )


def split_const(matrix):
    high = lax.reduce_precision(matrix, 8, 7)
    return high.astype(bf16), (matrix - high).astype(bf16)


def split_value(value):
    high = value.astype(bf16)
    return high, (value - high.astype(f32)).astype(bf16)


def dot3(a, b, contract=((1,), (0,))):
    dims = (contract, ((), ()))

    def one(x, y):
        return lax.dot_general(x, y, dims, preferred_element_type=f32)

    return one(a[0], b[0]) + one(a[0], b[1]) + one(a[1], b[0])


def full_spec(shape):
    zeros = (0,) * len(shape)
    return pl.BlockSpec(shape, lambda *_: zeros)


def lane_sign(half):
    lanes = lax.broadcasted_iota(jnp.int32, (1, 2 * half), 1)
    return jnp.where(lanes < half, -1.0, 1.0).astype(f32)


def rot(value, half):
    return pltpu.roll(value, half, axis=1) * lane_sign(half)


def y_matrix(width_y, modes, weights):
    step = 32
    count, half = modes.shape
    k = jnp.concatenate([modes, modes], axis=1).reshape(1, -1)
    phase = jnp.concatenate([jnp.zeros((count, half)), jnp.ones((count, half))], axis=1)
    phase = (0.5 * math.pi * phase).reshape(1, -1).astype(f32)
    unit = 2.0 * math.pi / width_y
    a = jnp.arange(width_y // step, dtype=jnp.int32)[:, None] * step
    b = jnp.arange(step, dtype=jnp.int32)[:, None]
    angle_a = unit * (a * k % width_y).astype(f32)
    angle_b = unit * (b * k % width_y).astype(f32) + phase
    w = jnp.concatenate([weights, weights], axis=1).reshape(1, -1) / math.sqrt(width_y)
    ca, sa = jnp.cos(angle_a) * w, jnp.sin(angle_a) * w
    cb, sb = jnp.cos(angle_b), jnp.sin(angle_b)
    ca, sa, cb, sb = lax.optimization_barrier((ca, sa, cb, sb))
    full = ca[:, None, :] * cb[None] - sa[:, None, :] * sb[None]
    return split_const(full.reshape(width_y, -1))


def z_angles(depth_z, rows_m, cols_z):
    return (
        2.0
        * math.pi
        / depth_z
        * (rows_m[:, None] * cols_z[None, :] % depth_z).astype(f32)
    )


def early_kernel(vel_ref, fh_ref, fl_ref, *outs):
    u = vel_ref[:, 0]
    c = -u[2][None] * u
    rows = u.shape[0] * u.shape[1]
    lhs = jnp.concatenate([u.reshape(rows, -1), c.reshape(rows, -1)], axis=0)
    res = dot3(split_value(lhs), (fh_ref[...], fl_ref[...]))
    at = 0
    for out in outs:
        width = out.shape[-1]
        piece = res[:, at : at + width]
        out[...] = piece.reshape(2, 3, 1, -1, width)
        at += width


def early_call(vel, f_pair, widths):
    _, X, Rz, NY = vel.shape
    shapes = [jax.ShapeDtypeStruct((2, 3, X, Rz, w), f32) for w in widths]
    return pl.pallas_call(
        early_kernel,
        grid=(X,),
        in_specs=[
            pl.BlockSpec((3, 1, Rz, NY), lambda x: (0, x, 0, 0)),
            full_spec(f_pair[0].shape),
            full_spec(f_pair[1].shape),
        ],
        out_specs=[pl.BlockSpec((2, 3, 1, Rz, w), lambda x: (0, 0, x, 0, 0)) for w in widths],
        out_shape=shapes,
        compiler_params=params(),
        name="early",
    )(vel, *f_pair)


def late_body(omega, half, n_out, bg_ref, vel_ref, left_ref, right_ref, fh_ref, fl_ref, vec_ref, *rest):
    uc_refs, outs, (ext_ref, ah_ref, al_ref) = rest[:n_out], rest[n_out : 2 * n_out], rest[2 * n_out :]
    X, Rz, NY = vel_ref.shape[1:]
    x = pl.program_id(0)

    @pl.when(x == 0)
    def _():
        ext_ref[:, 0:3] = left_ref[...]
        ext_ref[:, 3 : X + 3] = vel_ref[...]
        ext_ref[:, X + 3 :] = right_ref[...]

    d1 = (-1.0 / 60.0, 9.0 / 60.0, -45.0 / 60.0, 0.0, 45.0 / 60.0, -9.0 / 60.0, 1.0 / 60.0)
    d2 = tuple(v / 180.0 for v in (2.0, -27.0, 270.0, -490.0, 270.0, -27.0, 2.0))
    background = bg_ref[x]
    step = min(512, NY)

    def tile(r, carry):
        rows = pl.ds(r * 8, 8)
        for at in range(0, NY, step):
            cols = slice(at, at + step)
            acc = [None] * 3
            for o in range(7):
                u = [ext_ref[i, x + o, rows, cols] for i in range(3)]
                for i in range(3):
                    part = (viscosity * d2[o]) * u[i]
                    if d1[o] != 0.0:
                        part = part - d1[o] * (u[0] * u[i])
                    acc[i] = part if acc[i] is None else acc[i] + part
            u = [ext_ref[i, x + 3, rows, cols] for i in range(3)]
            acc[0] = acc[0] + 2.0 * omega * u[1]
            acc[1] = acc[1] - (2.0 - shear_param) * omega * u[0]
            speed = -(u[1] + background)
            for i in range(3):
                for n, value in enumerate((acc[i], speed * u[i])):
                    hi = value.astype(bf16).astype(f32)
                    ah_ref[n, i, rows, cols] = hi
                    al_ref[n, i, rows, cols] = value - hi
        return carry

    lax.fori_loop(0, Rz // 8, tile, 0)
    rows = 3 * Rz
    lhs = (
        ah_ref[...].reshape(2 * rows, NY).astype(bf16),
        al_ref[...].reshape(2 * rows, NY).astype(bf16),
    )
    res = dot3(lhs, (fh_ref[...], fl_ref[...]))
    at = 0
    for uc, out in zip(uc_refs, outs):
        for j in range(out.shape[-1] // (2 * half)):
            cols = slice(at, at + 2 * half)
            own = slice(j * 2 * half, (j + 1) * 2 * half)
            ky = vec_ref[0:1, cols]
            yu = uc[0, :, 0, :, own].reshape(rows, 2 * half)
            w = res[:rows, cols] + ky * rot(res[rows:, cols], half) - (viscosity * ky * ky) * yu
            out[:, 0, :, own] = w.reshape(3, Rz, 2 * half)
            at += 2 * half


def late_call(vel, left, right, background, omega, f_pair, vec, uc, half):
    _, X, Rz, NY = vel.shape
    widths = [u.shape[-1] for u in uc]
    n_out = len(uc)
    return pl.pallas_call(
        lambda *refs: late_body(omega, half, n_out, *refs),
        grid=(X,),
        in_specs=[
            pl.BlockSpec(memory_space=pltpu.SMEM),
            full_spec(vel.shape),
            full_spec(left.shape),
            full_spec(right.shape),
            full_spec(f_pair[0].shape),
            full_spec(f_pair[1].shape),
            full_spec(vec.shape),
        ]
        + [pl.BlockSpec((1, 3, 1, Rz, w), lambda x: (0, 0, x, 0, 0)) for w in widths],
        out_specs=[pl.BlockSpec((3, 1, Rz, w), lambda x: (0, x, 0, 0)) for w in widths],
        out_shape=[jax.ShapeDtypeStruct((3, X, Rz, w), f32) for w in widths],
        scratch_shapes=[
            pltpu.VMEM((3, X + 6, Rz, NY), f32),
            pltpu.VMEM((2, 3, Rz, NY), f32),
            pltpu.VMEM((2, 3, Rz, NY), f32),
        ],
        compiler_params=params(),
        name="late",
    )(background, vel, left, right, *f_pair, vec, *uc)


def z_body(n_src, n_t, half, mh_ref, ml_ref, *rest):
    ucs, ws = rest[:n_src], rest[n_src : 2 * n_src]
    outs, buf = rest[2 * n_src : 2 * n_src + n_t], rest[-1]
    X, Rz = ws[0].shape[1:3]
    wide = 2 * half
    depth = outs[0].shape[2]
    for t in range(n_t):
        own = slice(t * wide, (t + 1) * wide)
        at = 0
        for f in range(3):
            for s in range(n_src):
                for x in range(X):
                    piece = ws[s][0, x, :, own] if f == 2 else ucs[s][f, 0, x, :, own]
                    col = (t * X + x) * wide
                    buf[at : at + Rz, col : col + wide] = piece
                at += Rz
    res = dot3((mh_ref[...], ml_ref[...]), split_value(buf[...]))
    for t in range(n_t):
        for x in range(X):
            col = (t * X + x) * wide
            cols = slice(col, col + wide)
            outs[t][0, x] = res[:depth, cols] + rot(res[depth:, cols], half)


def z_call(m_pair, ucs, ws, n_t, half):
    _, X, Rz, width = ws[0].shape
    depth = m_pair[0].shape[0] // 2
    n_src = len(ws)
    return pl.pallas_call(
        lambda *refs: z_body(n_src, n_t, half, *refs),
        grid=(3,),
        in_specs=[full_spec(m_pair[0].shape)] * 2
        + [pl.BlockSpec((2, 1, X, Rz, width), lambda i: (0, i, 0, 0, 0))] * n_src
        + [pl.BlockSpec((1, X, Rz, width), lambda i: (i, 0, 0, 0))] * n_src,
        out_specs=[pl.BlockSpec((1, X, depth, 2 * half), lambda i: (i, 0, 0, 0))] * n_t,
        out_shape=[jax.ShapeDtypeStruct((3, X, depth, 2 * half), f32)] * n_t,
        scratch_shapes=[pltpu.VMEM((3 * n_src * Rz, n_t * X * 2 * half), f32)],
        compiler_params=params(),
        name="zforward",
    )(*m_pair, *ucs, *ws)


def prep_body(n_part, half, vec_ref, kz_ref, *rest):
    parts = rest[:n_part]
    tend, dsum, up, down = rest[n_part:]
    X, depth = tend.shape[1:3]
    ky = vec_ref[0:1]

    def tile(r, carry):
        rows = pl.ds(r * 8, 8)
        kz = kz_ref[rows]
        for x in range(X):
            t = []
            for i in range(3):
                v = parts[0][i, x, rows]
                for p in parts[1:]:
                    v = v + p[i, x, rows]
                tend[i, x, rows] = v
                t.append(v)
            d = rot(ky * t[1] + kz * t[2], half)
            dsum[x, rows] = d
            if x < 3:
                down[x, rows] = t[0]
            if x >= X - 3:
                up[x - X + 3, rows] = t[0]
            if x < 2:
                down[3 + x, rows] = d
            if x >= X - 2:
                up[3 + x - X + 2, rows] = d
        return carry

    lax.fori_loop(0, depth // 8, tile, 0)


def prep_call(parts, vec, kz, half):
    _, X, depth, wide = parts[0].shape
    n = len(parts)
    return pl.pallas_call(
        lambda *refs: prep_body(n, half, *refs),
        out_shape=[
            jax.ShapeDtypeStruct((3, X, depth, wide), f32),
            jax.ShapeDtypeStruct((X, depth, wide), f32),
            jax.ShapeDtypeStruct((5, depth, wide), f32),
            jax.ShapeDtypeStruct((5, depth, wide), f32),
        ],
        compiler_params=pltpu.CompilerParams(vmem_limit_bytes=VMEM_BYTES),
        name="prep",
    )(vec, kz, *parts)


def take_chunk(ref, lead, rows, chunk, half):
    total = ref.shape[-1]
    if total == 2 * half:
        return ref[lead + (rows,)]
    wide = 2 * half
    assert total == 2 * wide
    re = ref[lead + (rows, slice(0, wide))]
    im = ref[lead + (rows, slice(wide, total))]
    low = lax.broadcasted_iota(jnp.int32, (1, wide), 1) < half
    if chunk == 0:
        return jnp.where(low, re, pltpu.roll(im, half, axis=1))
    return jnp.where(low, pltpu.roll(re, half, axis=1), im)


def solve_body(chunk, half, n_slot, vec_ref, kz_ref, inv_ref, mh_ref, ml_ref, tend, dsum, fl, fr, p0, p0l, p0r, q_old, *rest):
    q_out, p_out = rest[:2]
    outs = rest[2 : 2 + n_slot]
    buf = rest[2 + n_slot]
    X, depth = tend.shape[1:3]
    wide = 2 * half
    ky = vec_ref[0:1]
    cl, sl = vec_ref[1:2], vec_ref[2:3]
    cr, sr = vec_ref[3:4], vec_ref[4:5]

    def tile(r, carry):
        rows = pl.ds(r * 8, 8)
        kz = kz_ref[rows]
        inv = inv_ref[rows]

        def left(v):
            return v * cl + rot(v, half) * sl

        def right(v):
            return v * cr + rot(v, half) * sr

        tx = {x: tend[0, x, rows] for x in range(X)}
        dd = {x: dsum[x, rows] for x in range(X)}
        pp = {x: take_chunk(p0, (x,), rows, chunk, half) for x in range(X)}
        for o in range(3):
            tx[o - 3] = left(fl[o, rows])
            tx[X + o] = right(fr[o, rows])
            pp[o - 3] = left(take_chunk(p0l, (o,), rows, chunk, half))
            pp[X + o] = right(take_chunk(p0r, (o,), rows, chunk, half))
        for o in range(2):
            dd[o - 2] = left(fl[3 + o, rows])
            dd[X + o] = right(fr[3 + o, rows])
        div = {x: 0.5 * (tx[x + 1] - tx[x - 1]) + dd[x] for x in range(-2, X + 2)}
        for sweep in range(SWEEPS):
            reach = SWEEPS - sweep
            pp = {
                x: (pp[x + 1] + pp[x - 1] - div[x]) * inv
                for x in range(-reach, X + reach)
            }
        return_p = pp
        raise_p = None
        return rows, kz, tx, return_p, raise_p

    def full(r, carry):
        rows, kz, tx, pp, _ = tile(r, carry)
        for x in range(X):
            p = pp[x]
            p_out[x, rows] = p
            ip = rot(p, half)
            grad = (0.5 * (pp[x + 1] - pp[x - 1]), ky * ip, kz * ip)
            for i in range(3):
                old = take_chunk(q_old, (i, x), rows, chunk, half)
                now = tx[x] if i == 0 else tend[i, x, rows]
                q = keep_weight * old + time_step * (now - grad[i])
                q_out[i, x, rows] = q
                buf[i, rows, x * wide : (x + 1) * wide] = q
        return carry

    lax.fori_loop(0, depth // 8, full, 0)
    Rz = depth // n_slot
    mats = (mh_ref[...], ml_ref[...])
    for i in range(3):
        res = dot3(mats, split_value(buf[i]))
        for x in range(X):
            cols = slice(x * wide, (x + 1) * wide)
            h = res[:depth, cols] + rot(res[depth:, cols], half)
            for s in range(n_slot):
                outs[s][i, x] = h[s * Rz : (s + 1) * Rz]


def solve_call(chunk, half, n_slot, vec, kz, inv, m_pair, tend, dsum, fl, fr, p0, p0l, p0r, q_old):
    _, X, depth, wide = tend.shape
    return pl.pallas_call(
        lambda *refs: solve_body(chunk, half, n_slot, *refs),
        out_shape=[
            jax.ShapeDtypeStruct((3, X, depth, wide), f32),
            jax.ShapeDtypeStruct((X, depth, wide), f32),
        ]
        + [jax.ShapeDtypeStruct((3, X, depth // n_slot, wide), f32)] * n_slot,
        scratch_shapes=[pltpu.VMEM((3, depth, X * wide), f32)],
        compiler_params=pltpu.CompilerParams(vmem_limit_bytes=VMEM_BYTES),
        name="solve",
    )(vec, kz, inv, *m_pair, tend, dsum, fl, fr, p0, p0l, p0r, q_old)


def back_body(n_slot, base_ref, gh_ref, gl_ref, *rest):
    hs, out = rest[:n_slot], rest[-1]
    _, _, Rz, wide = hs[0].shape
    lhs = jnp.concatenate([h[...].reshape(3 * Rz, wide) for h in hs], axis=1)
    res = dot3(split_value(lhs), (gh_ref[...], gl_ref[...]), ((1,), (1,)))
    out[...] = base_ref[...] + section_weight * res.reshape(out.shape)


def back_call(base, g_pair, hs):
    _, X, Rz, NY = base.shape
    wide = hs[0].shape[-1]
    plane = lambda w: pl.BlockSpec((3, 1, Rz, w), lambda x: (0, x, 0, 0))
    return pl.pallas_call(
        lambda *refs: back_body(len(hs), *refs),
        grid=(X,),
        in_specs=[plane(NY), full_spec(g_pair[0].shape), full_spec(g_pair[1].shape)]
        + [plane(wide)] * len(hs),
        out_specs=plane(NY),
        out_shape=jax.ShapeDtypeStruct(base.shape, f32),
        compiler_params=params(),
        name="back",
    )(base, *g_pair, *hs)


def pack_body(half, a_ref, b_ref, out):
    wide = 2 * half
    low = lax.broadcasted_iota(jnp.int32, (1, wide), 1) < half
    a, b = a_ref[0], b_ref[0]
    out[0, :, 0:wide] = jnp.where(low, a, pltpu.roll(b, half, axis=1))
    out[0, :, wide : 2 * wide] = jnp.where(low, pltpu.roll(a, half, axis=1), b)


def pack_call(chunks, half):
    if len(chunks) == 1:
        return chunks[0]
    a, b = chunks
    lead, (depth, wide) = a.shape[:-2], a.shape[-2:]
    n = math.prod(lead)
    spec = lambda w: pl.BlockSpec((1, depth, w), lambda i: (i, 0, 0))
    out = pl.pallas_call(
        lambda *refs: pack_body(half, *refs),
        grid=(n,),
        in_specs=[spec(wide), spec(wide)],
        out_specs=spec(2 * wide),
        out_shape=jax.ShapeDtypeStruct((n, depth, 2 * wide), f32),
        compiler_params=params(),
        name="pack",
    )(a.reshape(n, depth, wide), b.reshape(n, depth, wide))
    return out.reshape(lead + (depth, 2 * wide))


def ring(axis, shift):
    count = lax.axis_size(axis)
    return [(i, (i + shift) % count) for i in range(count)]


def local(vel, q_old, pressure_guess, shear_shift):
    X, Rz, NY = vel.shape[1:]
    depth = q_old.shape[2]
    G = lax.axis_size("yz")
    L = NY // (2 * G)
    half = 64 if L % 64 == 0 else L
    J = L // half
    g = lax.axis_index("yz")
    slab = lax.axis_index("gx")
    slabs = lax.axis_size("gx")
    total_x = X * slabs
    offset = shear_shift[0]
    omega = 2.0 / total_x
    paired = G == 4

    from_left = lax.ppermute(vel[:, X - 3 :], "gx", ring("gx", 1))
    from_right = lax.ppermute(vel[:, :3], "gx", ring("gx", -1))
    p_left = lax.ppermute(pressure_guess[X - 3 :], "gx", ring("gx", 1))
    p_right = lax.ppermute(pressure_guess[:3], "gx", ring("gx", -1))

    if paired:
        slot_groups = jnp.stack([g, G - 1 - g, g ^ 1, G - 1 - (g ^ 1)])
        sources = jnp.stack([g, g ^ 1])
        n_t = 2
    else:
        slot_groups = (g + jnp.arange(G, dtype=jnp.int32)) % G
        sources = (g - jnp.arange(G, dtype=jnp.int32)) % G
        n_t = 1
    back_groups = (g - jnp.arange(G, dtype=jnp.int32)) % G
    wide = 2 * half
    widths = [n_t * wide] * (2 if paired else G)

    def modes_of(groups, j):
        return groups[:, None] * L + j * half + jnp.arange(half, dtype=jnp.int32)[None, :]

    unit_y = 2.0 * math.pi / NY

    def twice(a):
        return jnp.concatenate([a, a], axis=-1).reshape(1, -1)

    m = jnp.arange(depth, dtype=jnp.int32)
    signed = jnp.where(m < depth // 2, m, m - depth)
    kz1 = 2.0 * math.pi / depth * signed.astype(f32)
    kz = jnp.broadcast_to(kz1[:, None], (depth, wide))
    zloc = jnp.arange(Rz, dtype=jnp.int32)
    z_cols = (sources[:, None] * Rz + zloc[None, :]).reshape(-1)
    ang = z_angles(depth, m, z_cols)
    norm_z = 1.0 / math.sqrt(depth)
    cz, sz = jnp.cos(ang) * norm_z, jnp.sin(ang) * norm_z
    kc = kz1[:, None]
    real = jnp.concatenate([-viscosity * kc * kc * cz, kc * sz, cz], axis=1)
    imag = jnp.concatenate([viscosity * kc * kc * sz, kc * cz, -sz], axis=1)
    m_fwd = split_const(jnp.concatenate([real, imag], axis=0))
    dest = (g + jnp.arange(G, dtype=jnp.int32)) % G
    z_rows = (dest[:, None] * Rz + zloc[None, :]).reshape(-1)
    ang_b = z_angles(depth, z_rows, m)
    m_inv = split_const(
        jnp.concatenate([jnp.cos(ang_b) * norm_z, jnp.sin(ang_b) * norm_z], axis=0)
    )

    def mix(rows, sign):
        return (1.0 - fraction) * jnp.roll(rows, sign * offset, axis=3) + fraction * jnp.roll(
            rows, sign * (offset + 1), axis=3
        )

    left = jnp.where(slab == 0, mix(from_left, -1), from_left)
    right = jnp.where(slab == slabs - 1, mix(from_right, 1), from_right)
    xpos = (slab * X + jnp.arange(X, dtype=jnp.int32)).astype(f32) + 0.5 - total_x / 2.0
    background = -shear_param * omega * xpos

    q_parts, p_parts = [], []
    result = vel
    for j in range(J):
        modes = modes_of(slot_groups, j)
        f_pair = y_matrix(NY, modes, jnp.ones(modes.shape, f32))
        ky_all = twice(unit_y * modes.astype(f32))
        uc = early_call(vel, f_pair, widths)
        w = late_call(vel, left, right, background, omega, f_pair, ky_all, uc, half)
        if paired:
            swap = [(i, i ^ 1) for i in range(G)]
            ucs = [uc[0], lax.ppermute(uc[1], "yz", swap)]
            ws = [w[0], lax.ppermute(w[1], "yz", swap)]
            mine, other = z_call(m_fwd, ucs, ws, n_t, half)
            parts = [mine, lax.ppermute(other, "yz", [(i, G - 1 - i) for i in range(G)])]
        else:
            ucs = [uc[0]] + [lax.ppermute(uc[s], "yz", ring("yz", s)) for s in range(1, G)]
            ws = [w[0]] + [lax.ppermute(w[s], "yz", ring("yz", s)) for s in range(1, G)]
            parts = z_call(m_fwd, ucs, ws, n_t, half)
        own = modes_of(g[None], j)
        ky = twice(unit_y * own.astype(f32))
        edge = unit_y * ((own * offset % NY).astype(f32) + fraction * own.astype(f32))
        ec, es = twice(jnp.cos(edge)), twice(jnp.sin(edge))
        first, last = slab == 0, slab == slabs - 1
        vec = jnp.concatenate(
            [
                ky,
                jnp.where(first, ec, 1.0),
                jnp.where(first, es, 0.0),
                jnp.where(last, ec, 1.0),
                jnp.where(last, -es, 0.0),
                jnp.zeros((3, wide), f32),
            ],
            axis=0,
        )
        inv = 1.0 / (2.0 + ky * ky + kz * kz)
        tend, dsum, up, down = prep_call(parts, vec, kz, half)
        fl = lax.ppermute(up, "gx", ring("gx", 1))
        fr = lax.ppermute(down, "gx", ring("gx", -1))
        q, p, *hs = solve_call(
            j, half, G, vec, kz, inv, m_inv, tend, dsum, fl, fr,
            pressure_guess, p_left, p_right, q_old,
        )
        q_parts.append(q)
        p_parts.append(p)
        got = [hs[0]] + [lax.ppermute(hs[s], "yz", ring("yz", s)) for s in range(1, G)]
        back_modes = modes_of(back_groups, j)
        weights = jnp.where(back_modes == 0, 1.0, 2.0).astype(f32)
        result = back_call(result, y_matrix(NY, back_modes, weights), got)
    return result, pack_call(q_parts, half), pack_call(p_parts, half)


def solution(mesh):
    placed = (P(None, "gx", "yz", None), P(None, "gx", None, "yz"), P("gx", None, "yz"), P())
    return jax.shard_map(
        local,
        mesh=mesh,
        in_specs=placed,
        out_specs=(P(None, "gx", "yz", None), P(None, "gx", None, "yz"), P("gx", None, "yz")),
        check_vma=False,
    )
```

```python
import math

import jax
import jax.numpy as jnp
from jax import lax
from jax.experimental import pallas as pl
from jax.experimental.pallas import tpu as pltpu
from jax.sharding import PartitionSpec as P


SWEEPS = 2
viscosity = 0.05
time_step = 0.2
keep_weight = -5.0 / 9.0
section_weight = 15.0 / 16.0
shear_param = 1.5
fraction = 0.375
f32 = jnp.float32
bf16 = jnp.bfloat16
COST_SCALE = 250_000_000


def params(mib, n=1):
    return pltpu.CompilerParams(
        vmem_limit_bytes=mib * 1024 * 1024, dimension_semantics=("arbitrary",) * n
    )


def cost(us):
    return pl.CostEstimate(flops=int(us * COST_SCALE), bytes_accessed=0, transcendentals=0)


def split_const(matrix):
    high = lax.reduce_precision(matrix, 8, 7)
    return high.astype(bf16), (matrix - high).astype(bf16)


def split_value(value):
    high = value.astype(bf16)
    return high, (value - high.astype(f32)).astype(bf16)


def dot3(a, b, contract=((1,), (0,))):
    dims = (contract, ((), ()))

    def one(x, y):
        return lax.dot_general(x, y, dims, preferred_element_type=f32)

    return one(a[0], b[0]) + one(a[0], b[1]) + one(a[1], b[0])


def full_spec(shape):
    zeros = (0,) * len(shape)
    return pl.BlockSpec(shape, lambda *_: zeros)


def lane_sign(half):
    lanes = lax.broadcasted_iota(jnp.int32, (1, 2 * half), 1)
    return jnp.where(lanes < half, -1.0, 1.0).astype(f32)


def rot(value, half):
    return pltpu.roll(value, half, axis=1) * lane_sign(half)


def y_matrix(width_y, modes, weights):
    step = 32
    count, half = modes.shape
    k = jnp.concatenate([modes, modes], axis=1).reshape(1, -1)
    phase = jnp.concatenate([jnp.zeros((count, half)), jnp.ones((count, half))], axis=1)
    phase = (0.5 * math.pi * phase).reshape(1, -1).astype(f32)
    unit = 2.0 * math.pi / width_y
    a = jnp.arange(width_y // step, dtype=jnp.int32)[:, None] * step
    b = jnp.arange(step, dtype=jnp.int32)[:, None]
    angle_a = unit * (a * k % width_y).astype(f32)
    angle_b = unit * (b * k % width_y).astype(f32) + phase
    w = jnp.concatenate([weights, weights], axis=1).reshape(1, -1) / math.sqrt(width_y)
    ca, sa = jnp.cos(angle_a) * w, jnp.sin(angle_a) * w
    cb, sb = jnp.cos(angle_b), jnp.sin(angle_b)
    ca, sa, cb, sb = lax.optimization_barrier((ca, sa, cb, sb))
    full = ca[:, None, :] * cb[None] - sa[:, None, :] * sb[None]
    return split_const(full.reshape(width_y, -1))


def z_angles(depth_z, rows_m, cols_z):
    return (
        2.0
        * math.pi
        / depth_z
        * (rows_m[:, None] * cols_z[None, :] % depth_z).astype(f32)
    )


def spectra_body(comp, omega, half, jobs, comps, n_out, bg_ref, *rest):
    vels = dict(zip(comps, rest))
    rest = rest[len(comps) :]
    ui, u0, u1, u2 = vels[comp], vels.get(0), vels.get(1), vels.get(2)
    has_w = any("w" in want for want in jobs)
    has_c = any("c" in want for want in jobs)
    if has_w:
        n_h = 2 if comp == 0 else 4
        halos, rest = rest[:n_h], rest[n_h:]
    mats, rest = rest[: 3 * len(jobs)], rest[3 * len(jobs) :]
    outs, buf = rest[:-1], rest[-1]
    _, X, Rz, NY = ui.shape
    d1 = (0.0, 45.0 / 60.0, -9.0 / 60.0, 1.0 / 60.0)
    d2 = (-490.0 / 180.0, 270.0 / 180.0, -27.0 / 180.0, 2.0 / 180.0)
    step = min(512, NY)
    base = 1 if has_c else 0

    def pick(i, at, rows, cols):
        if 0 <= at < X:
            return vels[i][0, at, rows, cols]
        ref = halos[(0 if i == 0 else 2) + (0 if at < 0 else 1)]
        return ref[0, at + 3 if at < 0 else at - X, rows, cols]

    def tile(r, carry):
        rows = pl.ds(pl.multiple_of(r * 8, 8), 8)
        for x in range(X):
            for at in range(0, NY, step):
                cols = slice(at, at + step)
                u = ui[0, x, rows, cols]
                if has_c:
                    buf[0, x, rows, cols] = -u2[0, x, rows, cols] * u
                buf[base, x, rows, cols] = u
                if has_w:
                    acc = (viscosity * d2[0]) * u
                    for o in (1, 2, 3):
                        up = pick(comp, x + o, rows, cols)
                        dn = pick(comp, x - o, rows, cols)
                        if comp == 0:
                            xp, xm = up, dn
                        else:
                            xp = pick(0, x + o, rows, cols)
                            xm = pick(0, x - o, rows, cols)
                        acc = acc + (viscosity * d2[o]) * (up + dn)
                        acc = acc - d1[o] * (xp * up - xm * dn)
                    if comp == 0:
                        acc = acc + (2.0 * omega) * u1[0, x, rows, cols]
                    if comp == 1:
                        acc = acc - ((2.0 - shear_param) * omega) * u0[0, x, rows, cols]
                    buf[base + 1, x, rows, cols] = acc
                    buf[base + 2, x, rows, cols] = -(u1[0, x, rows, cols] + bg_ref[x]) * u
        return carry

    lax.fori_loop(0, Rz // 8, tile, 0)
    M = X * Rz
    wide = 2 * half
    for n, want in enumerate(jobs):
        lo = 0 if "c" in want else base
        hi = base + (3 if "w" in want else 1)
        lhs = buf[lo:hi].reshape((hi - lo) * M, NY)
        res = dot3(split_value(lhs), (mats[3 * n][...], mats[3 * n + 1][...]))
        vec_ref = mats[3 * n + 2]
        u_at = (base - lo) * M
        at = 0
        for out in outs[n * n_out : (n + 1) * n_out]:
            for j in range(out.shape[-1] // wide):
                cols = slice(at, at + wide)
                own = slice(j * wide, (j + 1) * wide)
                yu = res[u_at : u_at + M, cols]
                if "c" in want:
                    out[0, :, :, own] = yu.reshape(X, Rz, wide)
                    out[1, :, :, own] = res[:M, cols].reshape(X, Rz, wide)
                if "w" in want:
                    k = u_at + M
                    ky = vec_ref[0:1, cols]
                    w = (
                        res[k : k + M, cols]
                        + ky * rot(res[k + M : k + 2 * M, cols], half)
                        - (viscosity * ky * ky) * yu
                    )
                    out[len(want) - 1, :, :, own] = w.reshape(X, Rz, wide)
                at += wide


def spectra_call(comp, jobs, vel, ghost, background, omega, mats, widths, half, us):
    _, X, Rz, NY = vel.shape
    has_w = any("w" in want for want in jobs)
    has_c = any("c" in want for want in jobs)
    comps = sorted({comp} | ({2} if has_c else set()) | ({0, 1} if has_w else set()))
    plane = lambda i: pl.BlockSpec((1, X, Rz, NY), lambda *_: (i, 0, 0, 0))
    halos, halo_specs = [], []
    if has_w:
        halos = list(ghost[0]) + (list(ghost[1]) if comp else [])
        block = (1,) + halos[0].shape[1:]
        halo_specs = [pl.BlockSpec(block, lambda *_: (0, 0, 0, 0))] * 2
        if comp:
            halo_specs += [pl.BlockSpec(block, lambda *_: (comp - 1, 0, 0, 0))] * 2
    count = (2 if has_c else 1) + (2 if has_w else 0)
    flat = [a for m in mats for a in m]
    shapes = [(len(want), X, Rz, w) for want in jobs for w in widths]
    return pl.pallas_call(
        lambda *refs: spectra_body(comp, omega, half, jobs, comps, len(widths), *refs),
        grid=(1,),
        in_specs=[pl.BlockSpec(memory_space=pltpu.SMEM)]
        + [plane(c) for c in comps]
        + halo_specs
        + [full_spec(a.shape) for a in flat],
        out_specs=[full_spec(shape) for shape in shapes],
        out_shape=[jax.ShapeDtypeStruct(shape, f32) for shape in shapes],
        scratch_shapes=[pltpu.VMEM((count, X, Rz, NY), f32)],
        compiler_params=params(50),
        cost_estimate=cost(us),
        name="spectra",
    )(background, *([vel] * len(comps)), *halos, *flat)


def z_body(counts, n_t, half, mh_ref, ml_ref, *rest):
    n_in = len(counts)
    ins, outs, buf = rest[:n_in], rest[n_in : n_in + n_t], rest[-1]
    _, X, Rz, _ = ins[0].shape
    wide = 2 * half
    depth = outs[0].shape[1]
    for t in range(n_t):
        own = slice(t * wide, (t + 1) * wide)
        at = 0
        for ref, count in zip(ins, counts):
            for f in range(count):
                for x in range(X):
                    col = (t * X + x) * wide
                    buf[at : at + Rz, col : col + wide] = ref[f, x, :, own]
                at += Rz
    res = dot3((mh_ref[...], ml_ref[...]), split_value(buf[...]))
    for t in range(n_t):
        for x in range(X):
            col = (t * X + x) * wide
            cols = slice(col, col + wide)
            outs[t][x] = res[:depth, cols] + rot(res[depth:, cols], half)


def z_call(m_pair, ins, n_t, half):
    flat = [a for source in ins for a in source]
    counts = [a.shape[0] for a in flat]
    _, X, Rz, _ = flat[0].shape
    depth = m_pair[0].shape[0] // 2
    return pl.pallas_call(
        lambda *refs: z_body(counts, n_t, half, *refs),
        out_shape=[jax.ShapeDtypeStruct((X, depth, 2 * half), f32)] * n_t,
        scratch_shapes=[pltpu.VMEM((sum(counts) * Rz, n_t * X * 2 * half), f32)],
        compiler_params=params(24, 0),
        cost_estimate=cost(4),
        name="zforward",
    )(*m_pair, *flat)


def shear_body(meta, up, down, up_out, down_out):
    NY = up.shape[-1]
    shift = meta[0]

    def one(flag, ref, out, by, by_next):
        @pl.when(flag == 1)
        def _():
            v = ref[0, 0]
            out[0, 0] = (1.0 - fraction) * pltpu.roll(v, by, 1) + fraction * pltpu.roll(v, by_next, 1)

        @pl.when(flag == 0)
        def _():
            out[0, 0] = ref[0, 0]

    one(meta[1], up, up_out, (NY - shift) % NY, (2 * NY - shift - 1) % NY)
    one(meta[2], down, down_out, shift % NY, (shift + 1) % NY)


def shear_call(meta, up, down):
    n, w, Rz, NY = up.shape
    spec = pl.BlockSpec((1, 1, Rz, NY), lambda i, x: (i, x, 0, 0))
    return pl.pallas_call(
        shear_body,
        grid=(n, w),
        in_specs=[pl.BlockSpec(memory_space=pltpu.SMEM), spec, spec],
        out_specs=[spec, spec],
        out_shape=[jax.ShapeDtypeStruct(up.shape, f32)] * 2,
        compiler_params=params(16, 2),
        cost_estimate=cost(3),
        name="shear",
    )(meta, up, down)


def blocks_of(depth):
    return 4 if depth % 32 == 0 else 1


def row_block(lead, rows, wide):
    zeros = (0,) * len(lead)
    return pl.BlockSpec(tuple(lead) + (rows, wide), lambda b: zeros + (b, 0))


def add_parts(parts, x, rows):
    v = parts[0][x, rows]
    for p in parts[1:]:
        v = v + p[x, rows]
    return v


def prep_body(n_part, half, vec_ref, kz_ref, *rest):
    parts = [rest[i * n_part : (i + 1) * n_part] for i in range(3)]
    up, down = rest[3 * n_part :]
    X, depth = parts[0][0].shape[:2]
    ky = vec_ref[0:1]

    def tile(r, carry):
        rows = pl.ds(pl.multiple_of(r * 8, 8), 8)
        kz = kz_ref[rows]
        for x in range(X):
            if x < 3 or x >= X - 3:
                t = add_parts(parts[0], x, rows)
                if x < 3:
                    down[x, rows] = t
                if x >= X - 3:
                    up[x - X + 3, rows] = t
            if x < 2 or x >= X - 2:
                d = rot(ky * add_parts(parts[1], x, rows) + kz * add_parts(parts[2], x, rows), half)
                if x < 2:
                    down[3 + x, rows] = d
                if x >= X - 2:
                    up[3 + x - X + 2, rows] = d
        return carry

    lax.fori_loop(0, depth // 8, tile, 0)


def prep_call(parts, vec, kz, half):
    X, depth, wide = parts[0][0].shape
    n = len(parts[0])
    nb = blocks_of(depth)
    rows = depth // nb
    flat = [a for p in parts for a in p]
    return pl.pallas_call(
        lambda *refs: prep_body(n, half, *refs),
        grid=(nb,),
        in_specs=[full_spec(vec.shape), row_block((), rows, wide)]
        + [row_block((X,), rows, wide)] * len(flat),
        out_specs=[row_block((5,), rows, wide)] * 2,
        out_shape=[jax.ShapeDtypeStruct((5, depth, wide), f32)] * 2,
        compiler_params=params(24),
        cost_estimate=cost(4),
        name="prep",
    )(vec, kz, *flat)


def take_chunk(ref, lead, rows, chunk, half):
    total = ref.shape[-1]
    if total == 2 * half:
        return ref[lead + (rows,)]
    wide = 2 * half
    assert total == 2 * wide
    re = ref[lead + (rows, slice(0, wide))]
    im = ref[lead + (rows, slice(wide, total))]
    low = lax.broadcasted_iota(jnp.int32, (1, wide), 1) < half
    if chunk == 0:
        return jnp.where(low, re, pltpu.roll(im, half, axis=1))
    return jnp.where(low, pltpu.roll(re, half, axis=1), im)


def solve_body(chunk, half, n_slot, n_part, nb, vec_ref, kz_ref, inv_ref, mh_ref, ml_ref, fl, fr, p0, p0l, p0r, q_old, *rest):
    parts = [rest[i * n_part : (i + 1) * n_part] for i in range(3)]
    rest = rest[3 * n_part :]
    q_out, p_out = rest[:2]
    outs, buf = rest[2:-1], rest[-1]
    X, depth = p_out.shape[:2]
    wide = 2 * half
    ky = vec_ref[0:1]
    cl, sl = vec_ref[1:2], vec_ref[2:3]
    cr, sr = vec_ref[3:4], vec_ref[4:5]
    step = pl.program_id(0)

    def left(v):
        return v * cl + rot(v, half) * sl

    def right(v):
        return v * cr + rot(v, half) * sr

    def tile(r, carry):
        rows = pl.ds(pl.multiple_of(r * 8, 8), 8)
        whole = pl.ds(pl.multiple_of(step * depth + r * 8, 8), 8)
        kz = kz_ref[rows]
        inv = inv_ref[rows]
        tx, ty, tz, dd, pp = {}, {}, {}, {}, {}
        for x in range(X):
            tx[x] = add_parts(parts[0], x, rows)
            ty[x] = add_parts(parts[1], x, rows)
            tz[x] = add_parts(parts[2], x, rows)
            dd[x] = rot(ky * ty[x] + kz * tz[x], half)
            pp[x] = take_chunk(p0, (x,), rows, chunk, half)
        for o in range(3):
            tx[o - 3] = left(fl[o, rows])
            tx[X + o] = right(fr[o, rows])
            pp[o - 3] = left(take_chunk(p0l, (o,), rows, chunk, half))
            pp[X + o] = right(take_chunk(p0r, (o,), rows, chunk, half))
        for o in range(2):
            dd[o - 2] = left(fl[3 + o, rows])
            dd[X + o] = right(fr[3 + o, rows])
        div = {x: 0.5 * (tx[x + 1] - tx[x - 1]) + dd[x] for x in range(-2, X + 2)}
        for sweep in range(SWEEPS):
            reach = SWEEPS - sweep
            pp = {
                x: (pp[x + 1] + pp[x - 1] - div[x]) * inv
                for x in range(-reach, X + reach)
            }
        for x in range(X):
            p = pp[x]
            p_out[x, rows] = p
            ip = rot(p, half)
            grad = (0.5 * (pp[x + 1] - pp[x - 1]), ky * ip, kz * ip)
            for i, now in enumerate((tx[x], ty[x], tz[x])):
                old = take_chunk(q_old, (i, x), rows, chunk, half)
                q = keep_weight * old + time_step * (now - grad[i])
                q_out[i, x, rows] = q
                buf[i, whole, x * wide : (x + 1) * wide] = q
        return carry

    lax.fori_loop(0, depth // 8, tile, 0)

    @pl.when(step == nb - 1)
    def _():
        total = depth * nb
        Rz = total // n_slot
        mats = (mh_ref[...], ml_ref[...])
        for i in range(3):
            res = dot3(mats, split_value(buf[i]))
            for x in range(X):
                cols = slice(x * wide, (x + 1) * wide)
                h = res[:total, cols] + rot(res[total:, cols], half)
                for s in range(n_slot):
                    piece = h[s * Rz : (s + 1) * Rz]
                    if len(outs) == n_slot:
                        outs[s][i, x] = piece
                    else:
                        outs[i * n_slot + s][0, x] = piece


def solve_call(chunk, half, n_slot, split, vec, kz, inv, m_pair, parts, fl, fr, p0, p0l, p0r, q_old):
    X, depth, wide = parts[0][0].shape
    nb = blocks_of(depth)
    rows = depth // nb
    n = len(parts[0])
    flat = [a for p in parts for a in p]
    packed = p0.shape[-1]
    lead = 1 if split else 3
    n_h = n_slot * (3 if split else 1)
    h_shape = (lead, X, depth // n_slot, wide)
    out = pl.pallas_call(
        lambda *refs: solve_body(chunk, half, n_slot, n, nb, *refs),
        grid=(nb,),
        in_specs=[
            full_spec(vec.shape),
            row_block((), rows, wide),
            row_block((), rows, wide),
            full_spec(m_pair[0].shape),
            full_spec(m_pair[1].shape),
            row_block((5,), rows, wide),
            row_block((5,), rows, wide),
            row_block((X,), rows, packed),
            row_block((3,), rows, packed),
            row_block((3,), rows, packed),
            row_block((3, X), rows, packed),
        ]
        + [row_block((X,), rows, wide)] * len(flat),
        out_specs=[row_block((3, X), rows, wide), row_block((X,), rows, wide)]
        + [full_spec(h_shape)] * n_h,
        out_shape=[
            jax.ShapeDtypeStruct((3, X, depth, wide), f32),
            jax.ShapeDtypeStruct((X, depth, wide), f32),
        ]
        + [jax.ShapeDtypeStruct(h_shape, f32)] * n_h,
        scratch_shapes=[pltpu.VMEM((3, depth, X * wide), f32)],
        compiler_params=params(40),
        cost_estimate=cost(10),
        name="solve",
    )(vec, kz, inv, *m_pair, fl, fr, p0, p0l, p0r, q_old, *flat)
    q, p, hs = out[0], out[1], list(out[2:])
    if split:
        return q, p, [hs[i * n_slot : (i + 1) * n_slot] for i in range(3)]
    return q, p, [hs]


def back_body(n_slot, base_ref, gh_ref, gl_ref, *rest):
    hs, out = rest[:n_slot], rest[-1]
    _, X, Rz, wide = hs[0].shape
    lhs = jnp.concatenate([h[...].reshape(X * Rz, wide) for h in hs], axis=1)
    res = dot3(split_value(lhs), (gh_ref[...], gl_ref[...]), ((1,), (1,)))
    out[...] = base_ref[...] + section_weight * res.reshape(out.shape)


def back_call(base, g_pair, hs, comp):
    _, X, Rz, NY = base.shape
    wide = hs[0].shape[-1]
    if comp is None:
        grid, at = (3,), lambda i: (i, 0, 0, 0)
        h_at = at
    else:
        grid, at = (1,), lambda i: (comp, 0, 0, 0)
        h_at = lambda i: (0, 0, 0, 0)
    return pl.pallas_call(
        lambda *refs: back_body(len(hs), *refs),
        grid=grid,
        in_specs=[pl.BlockSpec((1, X, Rz, NY), at), full_spec(g_pair[0].shape), full_spec(g_pair[1].shape)]
        + [pl.BlockSpec((1, X, Rz, wide), h_at)] * len(hs),
        out_specs=pl.BlockSpec((1, X, Rz, NY), at),
        out_shape=jax.ShapeDtypeStruct(base.shape, f32),
        input_output_aliases={} if comp is None else {0: 0},
        compiler_params=params(32),
        cost_estimate=cost(7),
        name="back",
    )(base, *g_pair, *hs)


def pack_body(half, a_ref, b_ref, out):
    wide = 2 * half
    low = lax.broadcasted_iota(jnp.int32, (1, wide), 1) < half
    for n in range(a_ref.shape[0]):
        a, b = a_ref[n], b_ref[n]
        out[n, :, 0:wide] = jnp.where(low, a, pltpu.roll(b, half, axis=1))
        out[n, :, wide : 2 * wide] = jnp.where(low, pltpu.roll(a, half, axis=1), b)


def pack_call(chunks, half):
    if len(chunks) == 1:
        return chunks[0]
    a, b = chunks
    lead, (depth, wide) = a.shape[:-2], a.shape[-2:]
    n = math.prod(lead)
    per = 3 if n % 3 == 0 else 1
    spec = lambda w: pl.BlockSpec((per, depth, w), lambda i: (i, 0, 0))
    out = pl.pallas_call(
        lambda *refs: pack_body(half, *refs),
        grid=(n // per,),
        in_specs=[spec(wide), spec(wide)],
        out_specs=spec(2 * wide),
        out_shape=jax.ShapeDtypeStruct((n, depth, 2 * wide), f32),
        compiler_params=params(16),
        cost_estimate=cost(5),
        name="pack",
    )(a.reshape(n, depth, wide), b.reshape(n, depth, wide))
    return out.reshape(lead + (depth, 2 * wide))


def ring(axis, shift):
    count = lax.axis_size(axis)
    return [(i, (i + shift) % count) for i in range(count)]


def after(value, *deps):
    return lax.optimization_barrier((value,) + deps)[0]


def local(vel, q_old, pressure_guess, shear_shift):
    X, Rz, NY = vel.shape[1:]
    depth = q_old.shape[2]
    G = lax.axis_size("yz")
    L = NY // (2 * G)
    half = 64 if L % 64 == 0 else L
    J = L // half
    wide = 2 * half
    g = lax.axis_index("yz")
    slab = lax.axis_index("gx")
    slabs = lax.axis_size("gx")
    total_x = X * slabs
    offset = shear_shift[0]
    omega = 2.0 / total_x
    paired = G == 4
    first, last = slab == 0, slab == slabs - 1

    if paired:
        slot_groups = jnp.stack([g, G - 1 - g, g ^ 1, G - 1 - (g ^ 1)])
        sources = jnp.stack([g, g ^ 1])
        n_t = 2
    else:
        slot_groups = (g + jnp.arange(G, dtype=jnp.int32)) % G
        sources = (g - jnp.arange(G, dtype=jnp.int32)) % G
        n_t = 1
    back_groups = (g - jnp.arange(G, dtype=jnp.int32)) % G
    widths = [n_t * wide] * (2 if paired else G)

    def modes_of(groups, j):
        return groups[:, None] * L + j * half + jnp.arange(half, dtype=jnp.int32)[None, :]

    unit_y = 2.0 * math.pi / NY

    def twice(a):
        return jnp.concatenate([a, a], axis=-1).reshape(1, -1)

    m = jnp.arange(depth, dtype=jnp.int32)
    signed = jnp.where(m < depth // 2, m, m - depth)
    kz1 = 2.0 * math.pi / depth * signed.astype(f32)
    kz = jnp.broadcast_to(kz1[:, None], (depth, wide))
    zloc = jnp.arange(Rz, dtype=jnp.int32)
    norm_z = 1.0 / math.sqrt(depth)
    kc = kz1[:, None]
    n_src = sources.shape[0]
    three = (n_src, 3, Rz)
    z_cols = jnp.broadcast_to((sources[:, None] * Rz + zloc[None, :])[:, None], three).reshape(-1)
    field = jnp.broadcast_to(jnp.arange(3, dtype=jnp.int32)[None, :, None], three).reshape(1, -1)
    ang = z_angles(depth, m, z_cols)
    cz, sz = jnp.cos(ang) * norm_z, jnp.sin(ang) * norm_z
    gain = jnp.where(field == 0, -viscosity * kc * kc, jnp.where(field == 1, kc, 1.0))
    real = gain * jnp.where(field == 1, sz, cz)
    imag = gain * jnp.where(field == 1, cz, -sz)
    m_fwd = split_const(jnp.concatenate([real, imag], axis=0))
    dest = (g + jnp.arange(G, dtype=jnp.int32)) % G
    z_rows = (dest[:, None] * Rz + zloc[None, :]).reshape(-1)
    ang_b = z_angles(depth, z_rows, m)
    m_inv = split_const(
        jnp.concatenate([jnp.cos(ang_b) * norm_z, jnp.sin(ang_b) * norm_z], axis=0)
    )
    xpos = (slab * X + jnp.arange(X, dtype=jnp.int32)).astype(f32) + 0.5 - total_x / 2.0
    background = -shear_param * omega * xpos

    f_pairs, kys = [], []
    for j in range(J):
        modes = modes_of(slot_groups, j)
        f_pairs.append(y_matrix(NY, modes, jnp.ones(modes.shape, f32)))
        kys.append(twice(unit_y * modes.astype(f32)))

    swap = [(i, i ^ 1) for i in range(G)]
    cross = [(i, G - 1 - i) for i in range(G)]

    def scatter(pieces):
        if paired:
            return [pieces[0], lax.ppermute(pieces[1], "yz", swap)]
        return [pieces[0]] + [
            lax.ppermute(pieces[s], "yz", ring("yz", s)) for s in range(1, len(pieces))
        ]

    token = []

    def chained(value):
        return after(value, *token) if token else value

    def mark(*arrays):
        token[:] = arrays

    def gather_z(sent):
        ins = [list(source) for source in zip(*sent)]
        got = z_call((chained(m_fwd[0]), m_fwd[1]), ins, n_t, half)
        mark(got[-1])
        if paired:
            return [got[0], lax.ppermute(got[1], "yz", cross)]
        return [got[0]]

    ghost = {}
    sends, parts, faces, solved = {}, {}, {}, {}
    meta = jnp.stack([offset, first.astype(jnp.int32), last.astype(jnp.int32)])

    def vel_halo(n, lo, hi):
        v = chained(vel)
        ghost[n] = (
            lax.ppermute(v[lo:hi, X - 3 :], "gx", ring("gx", 1)),
            lax.ppermute(v[lo:hi, :3], "gx", ring("gx", -1)),
        )

    def shear(n):
        ghost[n] = shear_call(chained(meta), *ghost[n])
        mark(*ghost[n])

    def spectra(i, *jobs, us=8):
        flat = spectra_call(
            i, [want for _, want in jobs], vel, ghost, chained(background), omega,
            [f_pairs[j] + (kys[j],) for j, _ in jobs], widths, half, us,
        )
        mark(flat[-1])
        n = len(widths)
        for at, (j, _) in enumerate(jobs):
            sends.setdefault((i, j), []).append(scatter(flat[at * n : (at + 1) * n]))

    def forward_z(i, j):
        parts[i, j] = gather_z(sends[i, j])

    p_halo = []

    def vectors(j):
        own = modes_of(g[None], j)
        ky = twice(unit_y * own.astype(f32))
        edge = unit_y * ((own * offset % NY).astype(f32) + fraction * own.astype(f32))
        ec, es = twice(jnp.cos(edge)), twice(jnp.sin(edge))
        vec = jnp.concatenate(
            [
                ky,
                jnp.where(first, ec, 1.0),
                jnp.where(first, es, 0.0),
                jnp.where(last, ec, 1.0),
                jnp.where(last, -es, 0.0),
                jnp.zeros((3, wide), f32),
            ],
            axis=0,
        )
        return vec, 1.0 / (2.0 + ky * ky + kz * kz)

    def prep(j):
        vec, inv = vectors(j)
        mine = [parts[i, j] for i in range(3)]
        up, down = prep_call(mine, chained(vec), kz, half)
        mark(up, down)
        faces[j] = (
            vec,
            inv,
            mine,
            lax.ppermute(up, "gx", ring("gx", 1)),
            lax.ppermute(down, "gx", ring("gx", -1)),
        )

    def solve(j, split):
        vec, inv, mine, fl, fr = faces[j]
        q, p, groups = solve_call(
            j, half, G, split, chained(vec), kz, inv, m_inv, mine, fl, fr,
            pressure_guess, p_halo[0], p_halo[1], q_old,
        )
        mark(q)
        solved[j] = (q, p, groups)

    def give_back(j):
        out = []
        for hs in solved[j][2]:
            got = [hs[0]]
            for s in range(1, G):
                got.append(lax.ppermute(hs[s], "yz", ring("yz", s)))
            out.append(got)
        return out

    def back_matrix(j):
        back_modes = modes_of(back_groups, j)
        weights = jnp.where(back_modes == 0, 1.0, 2.0).astype(f32)
        return y_matrix(NY, back_modes, weights)

    def guess_halo():
        guess = chained(pressure_guess)
        p_halo.append(lax.ppermute(guess[X - 3 :], "gx", ring("gx", 1)))
        p_halo.append(lax.ppermute(guess[:3], "gx", ring("gx", -1)))

    if J == 2:
        vel_halo(0, 0, 1)
        spectra(0, (0, "uc"), us=6)
        vel_halo(1, 1, 3)
        spectra(1, (0, "uc"), us=6)
        shear(0)
        spectra(0, (0, "w"))
        spectra(2, (0, "uc"), us=6)
        guess_halo()
        forward_z(0, 0)
        shear(1)
        spectra(1, (0, "w"))
        spectra(2, (0, "w"))
        forward_z(1, 0)
        spectra(0, (1, "ucw"))
        forward_z(2, 0)
        spectra(1, (1, "ucw"))
        forward_z(0, 1)
        spectra(2, (1, "ucw"))
        prep(0)
        forward_z(1, 1)
        solve(0, False)
        forward_z(2, 1)
        q, p, groups = solved[0]
        solved[0] = (q, p, [[chained(h) for h in hs] for hs in groups])
        got = give_back(0)
        prep(1)
        solve(1, False)
        got1 = give_back(1)
        base = chained(vel)
        result = back_call(base, back_matrix(0), got[0], None)
        result = back_call(result, back_matrix(1), got1[0], None)
    else:
        if J > 2:
            raise NotImplementedError
        guess_halo()
        vel_halo(0, 0, 1)
        vel_halo(1, 1, 3)
        shear(0)
        shear(1)
        result = vel
        for j in range(J):
            for i in range(3):
                spectra(i, (j, "ucw"))
                forward_z(i, j)
            prep(j)
            solve(j, False)
            result = back_call(result, back_matrix(j), give_back(j)[0], None)
    q_parts = [solved[j][0] for j in range(J)]
    p_parts = [solved[j][1] for j in range(J)]
    return result, pack_call(q_parts, half), pack_call(p_parts, half)


def solution(mesh):
    placed = (P(None, "gx", "yz", None), P(None, "gx", None, "yz"), P("gx", None, "yz"), P())
    return jax.shard_map(
        local,
        mesh=mesh,
        in_specs=placed,
        out_specs=(P(None, "gx", "yz", None), P(None, "gx", None, "yz"), P("gx", None, "yz")),
        check_vma=False,
    )
```

```python
import math

import jax
import jax.numpy as jnp
import numpy as np
from jax import lax
from jax.experimental import pallas as pl
from jax.experimental.pallas import tpu as pltpu
from jax.sharding import PartitionSpec as P


SWEEPS = 2
viscosity = 0.05
time_step = 0.2
keep_weight = -5.0 / 9.0
section_weight = 15.0 / 16.0
shear_param = 1.5
fraction = 0.375
f32 = jnp.float32
bf16 = jnp.bfloat16
COST_SCALE = 250_000_000


def params(mib, n=1):
    return pltpu.CompilerParams(
        vmem_limit_bytes=mib * 1024 * 1024, dimension_semantics=("arbitrary",) * n
    )


def cost(us):
    return pl.CostEstimate(flops=int(us * COST_SCALE), bytes_accessed=0, transcendentals=0)


def split_const(matrix):
    exact = matrix.astype(np.float32)
    high = exact.astype(jnp.bfloat16)
    low = (exact - high.astype(np.float32)).astype(jnp.bfloat16)
    return jnp.asarray(high), jnp.asarray(low)


def split_value(value):
    high = value.astype(bf16)
    return high, (value - high.astype(f32)).astype(bf16)


def dot3(a, b, contract=((1,), (0,))):
    dims = (contract, ((), ()))

    def one(x, y):
        return lax.dot_general(x, y, dims, preferred_element_type=f32)

    return one(a[0], b[0]) + one(a[0], b[1]) + one(a[1], b[0])


def full_spec(shape):
    zeros = (0,) * len(shape)
    return pl.BlockSpec(shape, lambda *_: zeros)


def lane_sign(half):
    lanes = lax.broadcasted_iota(jnp.int32, (1, 2 * half), 1)
    return jnp.where(lanes < half, -1.0, 1.0).astype(f32)


def rot(value, half):
    return pltpu.roll(value, half, axis=1) * lane_sign(half)


def y_matrix(width_y, modes):
    angle = 2.0 * np.pi / width_y * (np.arange(width_y)[:, None, None] * modes[None] % width_y)
    full = np.concatenate([np.cos(angle), -np.sin(angle)], axis=2)
    return split_const(full.reshape(width_y, -1) / math.sqrt(width_y))


def z_forward_matrix(depth, rows, sources):
    m = np.arange(depth)
    kz = (2.0 * np.pi / depth * np.where(m < depth // 2, m, m - depth))[:, None]
    blocks = []
    for source in sources:
        z = source * rows + np.arange(rows)
        wave = np.exp(-2j * np.pi / depth * (m[:, None] * z[None, :] % depth))
        blocks += [-viscosity * kz * kz * wave, 1j * kz * wave, wave]
    full = np.concatenate(blocks, axis=1) / math.sqrt(depth)
    return np.concatenate([full.real, full.imag], axis=0)


def z_inverse_matrix(depth):
    m = np.arange(depth)
    full = np.exp(2j * np.pi / depth * (m[:, None] * m[None, :] % depth)) / math.sqrt(depth)
    return split_const(np.concatenate([full.real, full.imag], axis=0))


def block_at(index, size):
    return pl.ds(pl.multiple_of(index * size, size), size)


def spectra_body(comp, omega, half, jobs, comps, n_out, ids, bg_ref, *rest):
    vels = dict(zip(comps, rest))
    rest = rest[len(comps) :]
    ui, u0, u1, u2 = vels[comp], vels.get(0), vels.get(1), vels.get(2)
    has_w = any("w" in want for want in jobs)
    has_c = any("c" in want for want in jobs)
    if has_w:
        n_h = 2 if comp == 0 else 4
        halos, rest = rest[:n_h], rest[n_h:]
    mats, rest = rest[: 3 * len(jobs)], rest[3 * len(jobs) :]
    outs, (buf, res) = rest[:-2], rest[-2:]
    _, X, Rz, NY = ui.shape
    d1 = (0.0, 45.0 / 60.0, -9.0 / 60.0, 1.0 / 60.0)
    d2 = (-490.0 / 180.0, 270.0 / 180.0, -27.0 / 180.0, 2.0 / 180.0)
    step = min(512, NY)
    base = 1 if has_c else 0

    def pick(i, at, rows, cols):
        if 0 <= at < X:
            return vels[i][0, at, rows, cols]
        ref = halos[(0 if i == 0 else 2) + (0 if at < 0 else 1)]
        return ref[0, at + 3 if at < 0 else at - X, rows, cols]

    def tile(r, carry):
        rows = pl.ds(pl.multiple_of(r // (NY // step) * 8, 8), 8)
        cols = pl.ds(pl.multiple_of(r % (NY // step) * step, step), step)
        for x in range(X):
            u = ui[0, x, rows, cols]
            if has_c:
                buf[0, x, rows, cols] = -u2[0, x, rows, cols] * u
            buf[base, x, rows, cols] = u
            if has_w:
                acc = (viscosity * d2[0]) * u
                for o in (1, 2, 3):
                    up = pick(comp, x + o, rows, cols)
                    dn = pick(comp, x - o, rows, cols)
                    if comp == 0:
                        xp, xm = up, dn
                    else:
                        xp = pick(0, x + o, rows, cols)
                        xm = pick(0, x - o, rows, cols)
                    acc = acc + (viscosity * d2[o]) * (up + dn)
                    acc = acc - d1[o] * (xp * up - xm * dn)
                if comp == 0:
                    acc = acc + (2.0 * omega) * u1[0, x, rows, cols]
                if comp == 1:
                    acc = acc - ((2.0 - shear_param) * omega) * u0[0, x, rows, cols]
                buf[base + 1, x, rows, cols] = acc
                buf[base + 2, x, rows, cols] = -(u1[0, x, rows, cols] + bg_ref[x]) * u
        return carry

    lax.fori_loop(0, Rz // 8 * (NY // step), tile, 0)
    M = X * Rz
    wide = 2 * half
    for n, want in enumerate(jobs):
        lo = 0 if "c" in want else base
        hi = base + (3 if "w" in want else 1)
        high, low, vec_ref = mats[3 * n : 3 * n + 3]

        def product(f, carry):
            lhs = split_value(buf[f].reshape(M, NY))
            res[f] = dot3(lhs, (high[...], low[...]))
            return carry

        lax.fori_loop(lo, hi, product, 0)
        slot = 0
        for out in outs[n * n_out : (n + 1) * n_out]:
            for j in range(out.shape[-1] // wide):
                cols = block_at(ids[slot], wide)
                own = slice(j * wide, (j + 1) * wide)
                yu = res[base, :, cols]
                if "c" in want:
                    out[0, :, :, own] = yu.reshape(X, Rz, wide)
                    out[1, :, :, own] = res[0, :, cols].reshape(X, Rz, wide)
                if "w" in want:
                    ky = vec_ref[0:1, cols]
                    w = (
                        res[base + 1, :, cols]
                        + ky * rot(res[base + 2, :, cols], half)
                        - (viscosity * ky * ky) * yu
                    )
                    out[len(want) - 1, :, :, own] = w.reshape(X, Rz, wide)
                slot += 1


def spectra_call(comp, jobs, vel, ghost, ids, background, omega, mats, widths, half, us):
    _, X, Rz, NY = vel.shape
    has_w = any("w" in want for want in jobs)
    has_c = any("c" in want for want in jobs)
    comps = sorted({comp} | ({2} if has_c else set()) | ({0, 1} if has_w else set()))
    plane = lambda i: pl.BlockSpec((1, X, Rz, NY), lambda *_: (i, 0, 0, 0))
    halos, halo_specs = [], []
    if has_w:
        halos = list(ghost[0]) + (list(ghost[1]) if comp else [])
        block = (1,) + halos[0].shape[1:]
        halo_specs = [pl.BlockSpec(block, lambda *_: (0, 0, 0, 0))] * 2
        if comp:
            halo_specs += [pl.BlockSpec(block, lambda *_: (comp - 1, 0, 0, 0))] * 2
    count = (2 if has_c else 1) + (2 if has_w else 0)
    flat = [a for m in mats for a in m]
    shapes = [(len(want), X, Rz, w) for want in jobs for w in widths]
    return pl.pallas_call(
        lambda *refs: spectra_body(comp, omega, half, jobs, comps, len(widths), *refs),
        grid=(1,),
        in_specs=[pl.BlockSpec(memory_space=pltpu.SMEM)] * 2
        + [plane(c) for c in comps]
        + halo_specs
        + [full_spec(a.shape) for a in flat],
        out_specs=[full_spec(shape) for shape in shapes],
        out_shape=[jax.ShapeDtypeStruct(shape, f32) for shape in shapes],
        scratch_shapes=[
            pltpu.VMEM((count, X, Rz, NY), f32),
            pltpu.VMEM((count, X * Rz, sum(widths)), f32),
        ],
        compiler_params=params(50),
        cost_estimate=cost(us),
        name="spectra",
    )(ids, background, *([vel] * len(comps)), *halos, *flat)


def z_body(counts, first_id, n_t, half, ids, mh_ref, ml_ref, *rest):
    n_in = len(counts)
    ins, outs, buf = rest[:n_in], rest[n_in : n_in + n_t], rest[-1]
    _, X, Rz, _ = ins[0].shape
    wide = 2 * half
    depth = outs[0].shape[1]
    for t in range(n_t):
        own = slice(t * wide, (t + 1) * wide)
        n = 0
        for ref, count in zip(ins, counts):
            for f in range(count):
                rows = block_at(ids[first_id + n // 3] * 3 + n % 3, Rz)
                for x in range(X):
                    col = (t * X + x) * wide
                    buf[rows, col : col + wide] = ref[f, x, :, own]
                n += 1
    res = dot3((mh_ref[...], ml_ref[...]), split_value(buf[...]))
    for t in range(n_t):
        for x in range(X):
            col = (t * X + x) * wide
            cols = slice(col, col + wide)
            outs[t][x] = res[:depth, cols] + rot(res[depth:, cols], half)


def z_call(m_pair, ids, first_id, ins, n_t, half):
    flat = [a for source in ins for a in source]
    counts = [a.shape[0] for a in flat]
    _, X, Rz, _ = flat[0].shape
    depth = m_pair[0].shape[0] // 2
    return pl.pallas_call(
        lambda *refs: z_body(counts, first_id, n_t, half, *refs),
        in_specs=[pl.BlockSpec(memory_space=pltpu.SMEM)]
        + [pl.BlockSpec(memory_space=pltpu.VMEM)] * (2 + len(flat)),
        out_shape=[jax.ShapeDtypeStruct((X, depth, 2 * half), f32)] * n_t,
        scratch_shapes=[pltpu.VMEM((sum(counts) * Rz, n_t * X * 2 * half), f32)],
        compiler_params=params(24, 0),
        cost_estimate=cost(4),
        name="zforward",
    )(ids, *m_pair, *flat)


def shear_body(meta, up, down, up_out, down_out):
    NY = up.shape[-1]
    shift = meta[0]

    def one(flag, ref, out, by, by_next):
        @pl.when(flag == 1)
        def _():
            v = ref[0, 0]
            out[0, 0] = (1.0 - fraction) * pltpu.roll(v, by, 1) + fraction * pltpu.roll(v, by_next, 1)

        @pl.when(flag == 0)
        def _():
            out[0, 0] = ref[0, 0]

    one(meta[1], up, up_out, (NY - shift) % NY, (2 * NY - shift - 1) % NY)
    one(meta[2], down, down_out, shift % NY, (shift + 1) % NY)


def shear_call(meta, up, down):
    n, w, Rz, NY = up.shape
    spec = pl.BlockSpec((1, 1, Rz, NY), lambda i, x: (i, x, 0, 0))
    return pl.pallas_call(
        shear_body,
        grid=(n, w),
        in_specs=[pl.BlockSpec(memory_space=pltpu.SMEM), spec, spec],
        out_specs=[spec, spec],
        out_shape=[jax.ShapeDtypeStruct(up.shape, f32)] * 2,
        compiler_params=params(16, 2),
        cost_estimate=cost(3),
        name="shear",
    )(meta, up, down)


def blocks_of(depth):
    return 4 if depth % 32 == 0 else 1


def row_block(lead, rows, wide):
    zeros = (0,) * len(lead)
    return pl.BlockSpec(tuple(lead) + (rows, wide), lambda b: zeros + (b, 0))


def add_parts(parts, x, rows):
    v = parts[0][x, rows]
    for p in parts[1:]:
        v = v + p[x, rows]
    return v


def cut(refs, counts):
    out, at = [], 0
    for n in counts:
        out.append(refs[at : at + n])
        at += n
    return out, refs[at:]


def prep_body(counts, half, vec_ref, kz_ref, *rest):
    parts, (up, down) = cut(rest, counts)
    X, depth = parts[0][0].shape[:2]
    ky = vec_ref[0:1]

    def tile(r, carry):
        rows = pl.ds(pl.multiple_of(r * 8, 8), 8)
        kz = kz_ref[rows]
        for x in range(X):
            if x < 3 or x >= X - 3:
                t = add_parts(parts[0], x, rows)
                if x < 3:
                    down[x, rows] = t
                if x >= X - 3:
                    up[x - X + 3, rows] = t
            if x < 2 or x >= X - 2:
                d = rot(ky * add_parts(parts[1], x, rows) + kz * add_parts(parts[2], x, rows), half)
                if x < 2:
                    down[3 + x, rows] = d
                if x >= X - 2:
                    up[3 + x - X + 2, rows] = d
        return carry

    lax.fori_loop(0, depth // 8, tile, 0)


def prep_call(parts, vec, kz, half):
    X, depth, wide = parts[0][0].shape
    n = [len(p) for p in parts]
    nb = blocks_of(depth)
    rows = depth // nb
    flat = [a for p in parts for a in p]
    return pl.pallas_call(
        lambda *refs: prep_body(n, half, *refs),
        grid=(nb,),
        in_specs=[full_spec(vec.shape), row_block((), rows, wide)]
        + [row_block((X,), rows, wide)] * len(flat),
        out_specs=[row_block((5,), rows, wide)] * 2,
        out_shape=[jax.ShapeDtypeStruct((5, depth, wide), f32)] * 2,
        compiler_params=params(24),
        cost_estimate=cost(4),
        name="prep",
    )(vec, kz, *flat)


def take_chunk(ref, lead, rows, chunk, half):
    total = ref.shape[-1]
    if total == 2 * half:
        return ref[lead + (rows,)]
    wide = 2 * half
    assert total == 2 * wide
    re = ref[lead + (rows, slice(0, wide))]
    im = ref[lead + (rows, slice(wide, total))]
    low = lax.broadcasted_iota(jnp.int32, (1, wide), 1) < half
    if chunk == 0:
        return jnp.where(low, re, pltpu.roll(im, half, axis=1))
    return jnp.where(low, pltpu.roll(re, half, axis=1), im)


def solve_body(chunk, half, n_slot, counts, nb, ids, vec_ref, kz_ref, inv_ref, mh_ref, ml_ref, fl, fr, p0, p0l, p0r, q_old, *rest):
    parts, rest = cut(rest, counts)
    q_out, p_out = rest[:2]
    outs, buf = rest[2:-1], rest[-1]
    X, depth = p_out.shape[:2]
    wide = 2 * half
    ky = vec_ref[0:1]
    cl, sl = vec_ref[1:2], vec_ref[2:3]
    cr, sr = vec_ref[3:4], vec_ref[4:5]
    step = pl.program_id(0)

    def left(v):
        return v * cl + rot(v, half) * sl

    def right(v):
        return v * cr + rot(v, half) * sr

    def tile(r, carry):
        rows = pl.ds(pl.multiple_of(r * 8, 8), 8)
        whole = pl.ds(pl.multiple_of(step * depth + r * 8, 8), 8)
        kz = kz_ref[rows]
        inv = inv_ref[rows]
        tx, ty, tz, dd, pp = {}, {}, {}, {}, {}
        for x in range(X):
            tx[x] = add_parts(parts[0], x, rows)
            ty[x] = add_parts(parts[1], x, rows)
            tz[x] = add_parts(parts[2], x, rows)
            dd[x] = rot(ky * ty[x] + kz * tz[x], half)
            pp[x] = take_chunk(p0, (x,), rows, chunk, half)
        for o in range(3):
            tx[o - 3] = left(fl[o, rows])
            tx[X + o] = right(fr[o, rows])
            pp[o - 3] = left(take_chunk(p0l, (o,), rows, chunk, half))
            pp[X + o] = right(take_chunk(p0r, (o,), rows, chunk, half))
        for o in range(2):
            dd[o - 2] = left(fl[3 + o, rows])
            dd[X + o] = right(fr[3 + o, rows])
        div = {x: 0.5 * (tx[x + 1] - tx[x - 1]) + dd[x] for x in range(-2, X + 2)}
        for sweep in range(SWEEPS):
            reach = SWEEPS - sweep
            pp = {
                x: (pp[x + 1] + pp[x - 1] - div[x]) * inv
                for x in range(-reach, X + reach)
            }
        for x in range(X):
            p = pp[x]
            p_out[x, rows] = p
            ip = rot(p, half)
            grad = (0.5 * (pp[x + 1] - pp[x - 1]), ky * ip, kz * ip)
            for i, now in enumerate((tx[x], ty[x], tz[x])):
                old = take_chunk(q_old, (i, x), rows, chunk, half)
                q = keep_weight * old + time_step * (now - grad[i])
                q_out[i, x, rows] = q
                buf[i, whole, x * wide : (x + 1) * wide] = q
        return carry

    lax.fori_loop(0, depth // 8, tile, 0)

    @pl.when(step == nb - 1)
    def _():
        total = depth * nb
        Rz = total // n_slot
        mats = (mh_ref[...], ml_ref[...])
        for i in range(3):
            res = dot3(mats, split_value(buf[i]))
            for x in range(X):
                cols = slice(x * wide, (x + 1) * wide)
                buf[i, :, cols] = (res[:total, cols] + rot(res[total:, cols], half)) * vec_ref[5:6]
            for s in range(n_slot):
                rows = block_at(ids[2 * n_slot + 2 + s], Rz)
                for x in range(X):
                    outs[s][i, x] = buf[i, rows, x * wide : (x + 1) * wide]


def solve_call(chunk, half, n_slot, ids, vec, kz, inv, m_pair, parts, fl, fr, p0, p0l, p0r, q_old):
    X, depth, wide = parts[0][0].shape
    nb = blocks_of(depth)
    rows = depth // nb
    n = [len(p) for p in parts]
    flat = [a for p in parts for a in p]
    packed = p0.shape[-1]
    n_h = n_slot
    h_shape = (3, X, depth // n_slot, wide)
    out = pl.pallas_call(
        lambda *refs: solve_body(chunk, half, n_slot, n, nb, *refs),
        grid=(nb,),
        in_specs=[
            pl.BlockSpec(memory_space=pltpu.SMEM),
            full_spec(vec.shape),
            row_block((), rows, wide),
            row_block((), rows, wide),
            full_spec(m_pair[0].shape),
            full_spec(m_pair[1].shape),
            row_block((5,), rows, wide),
            row_block((5,), rows, wide),
            row_block((X,), rows, packed),
            row_block((3,), rows, packed),
            row_block((3,), rows, packed),
            row_block((3, X), rows, packed),
        ]
        + [row_block((X,), rows, wide)] * len(flat),
        out_specs=[row_block((3, X), rows, wide), row_block((X,), rows, wide)]
        + [full_spec(h_shape)] * n_h,
        out_shape=[
            jax.ShapeDtypeStruct((3, X, depth, wide), f32),
            jax.ShapeDtypeStruct((X, depth, wide), f32),
        ]
        + [jax.ShapeDtypeStruct(h_shape, f32)] * n_h,
        scratch_shapes=[pltpu.VMEM((3, depth, X * wide), f32)],
        compiler_params=params(40),
        cost_estimate=cost(10),
        name="solve",
    )(ids, vec, kz, inv, *m_pair, fl, fr, p0, p0l, p0r, q_old, *flat)
    return out[0], out[1], [list(out[2:])]


def back_body(n_slot, ids, base_ref, gh_ref, gl_ref, *rest):
    hs, (out, buf) = rest[:n_slot], rest[n_slot:]
    _, X, Rz, wide = hs[0].shape
    for s, h in enumerate(hs):
        buf[:, block_at(ids[3 * n_slot + 2 + s], wide)] = h[...].reshape(X * Rz, wide)
    res = dot3(split_value(buf[...]), (gh_ref[...], gl_ref[...]), ((1,), (1,)))
    out[...] = base_ref[...] + section_weight * res.reshape(out.shape)


def back_call(base, g_pair, ids, hs):
    _, X, Rz, NY = base.shape
    wide = hs[0].shape[-1]
    plane = lambda w: pl.BlockSpec((1, X, Rz, w), lambda i: (i, 0, 0, 0))
    return pl.pallas_call(
        lambda *refs: back_body(len(hs), *refs),
        grid=(3,),
        in_specs=[
            pl.BlockSpec(memory_space=pltpu.SMEM),
            plane(NY),
            full_spec(g_pair[0].shape),
            full_spec(g_pair[1].shape),
        ]
        + [plane(wide)] * len(hs),
        out_specs=plane(NY),
        out_shape=jax.ShapeDtypeStruct(base.shape, f32),
        scratch_shapes=[pltpu.VMEM((X * Rz, len(hs) * wide), f32)],
        compiler_params=params(32),
        cost_estimate=cost(7),
        name="back",
    )(ids, base, *g_pair, *hs)


def pack_body(half, a_ref, b_ref, out):
    wide = 2 * half
    low = lax.broadcasted_iota(jnp.int32, (1, wide), 1) < half
    for n in range(a_ref.shape[0]):
        a, b = a_ref[n], b_ref[n]
        out[n, :, 0:wide] = jnp.where(low, a, pltpu.roll(b, half, axis=1))
        out[n, :, wide : 2 * wide] = jnp.where(low, pltpu.roll(a, half, axis=1), b)


def pack_call(chunks, half):
    if len(chunks) == 1:
        return chunks[0]
    a, b = chunks
    lead, (depth, wide) = a.shape[:-2], a.shape[-2:]
    n = math.prod(lead)
    per = 3 if n % 3 == 0 else 1
    spec = lambda w: pl.BlockSpec((per, depth, w), lambda i: (i, 0, 0))
    out = pl.pallas_call(
        lambda *refs: pack_body(half, *refs),
        grid=(n // per,),
        in_specs=[spec(wide), spec(wide)],
        out_specs=spec(2 * wide),
        out_shape=jax.ShapeDtypeStruct((n, depth, 2 * wide), f32),
        compiler_params=params(16),
        cost_estimate=cost(5),
        name="pack",
    )(a.reshape(n, depth, wide), b.reshape(n, depth, wide))
    return out.reshape(lead + (depth, 2 * wide))


def ring(axis, shift):
    count = lax.axis_size(axis)
    return [(i, (i + shift) % count) for i in range(count)]


def after(value, *deps):
    return lax.optimization_barrier((value,) + deps)[0]


def local(vel, q_old, pressure_guess, shear_shift):
    X, Rz, NY = vel.shape[1:]
    depth = q_old.shape[2]
    G = lax.axis_size("yz")
    L = NY // (2 * G)
    half = 64 if L % 64 == 0 else L
    J = L // half
    wide = 2 * half
    g = lax.axis_index("yz")
    slab = lax.axis_index("gx")
    slabs = lax.axis_size("gx")
    total_x = X * slabs
    offset = shear_shift[0]
    omega = 2.0 / total_x
    paired = G == 4
    first, last = slab == 0, slab == slabs - 1

    if paired:
        slot_groups = jnp.stack([g, G - 1 - g, g ^ 1, G - 1 - (g ^ 1)])
        slot_sources = slot_groups
    else:
        slot_groups = (g + jnp.arange(G, dtype=jnp.int32)) % G
        slot_sources = (g - jnp.arange(G, dtype=jnp.int32)) % G
    back_groups = (g - jnp.arange(G, dtype=jnp.int32)) % G

    def modes_of(groups, j):
        return groups[:, None] * L + j * half + jnp.arange(half, dtype=jnp.int32)[None, :]

    unit_y = 2.0 * math.pi / NY

    def twice(a):
        return jnp.concatenate([a, a], axis=-1).reshape(1, -1)

    m = jnp.arange(depth, dtype=jnp.int32)
    signed = jnp.where(m < depth // 2, m, m - depth)
    kz1 = 2.0 * math.pi / depth * signed.astype(f32)
    kz = jnp.broadcast_to(kz1[:, None], (depth, wide))
    m_inv = z_inverse_matrix(depth)
    m_direct = split_const(z_forward_matrix(depth, Rz, range(G)))
    pair_at = jnp.stack([g % 2, 1 - g % 2])
    if paired:
        halves = [split_const(z_forward_matrix(depth, Rz, (n, n + 1))) for n in (0, 2)]
        m_pair = [jnp.where(g < 2, low, high) for low, high in zip(*halves)]
    dest = (g + jnp.arange(G, dtype=jnp.int32)) % G
    ids = jnp.concatenate([slot_groups, slot_sources, pair_at, dest, back_groups])
    xpos = (slab * X + jnp.arange(X, dtype=jnp.int32)).astype(f32) + 0.5 - total_x / 2.0
    background = -shear_param * omega * xpos

    f_pairs, kys = [], []
    for j in range(J):
        modes = np.arange(G)[:, None] * L + j * half + np.arange(half)[None, :]
        f_pairs.append(y_matrix(NY, modes))
        both = np.concatenate([modes, modes], axis=1).reshape(1, -1)
        kys.append(jnp.asarray((unit_y * both).astype(np.float32)))

    swap = [(i, i ^ 1) for i in range(G)]
    cross = [(i, G - 1 - i) for i in range(G)]
    if paired:
        slot_perms = [None, cross, swap, ring("yz", 2)]
    else:
        slot_perms = [ring("yz", s) for s in range(G)]

    def direct(j):
        return not paired or j == 0

    def widths_of(j):
        return [wide] * G if direct(j) else [2 * wide] * 2

    def scatter(pieces, j):
        perms = slot_perms if direct(j) else [None, swap]
        order = [2, 3, 1] if paired and direct(j) else range(1, len(pieces))
        out = [pieces[0]] + [None] * (len(pieces) - 1)
        for s in order:
            out[s] = lax.ppermute(pieces[s], "yz", perms[s])
        return out

    token = []

    def chained(value):
        return after(value, *token) if token else value

    def mark(*arrays):
        token[:] = arrays

    def gather_z(sent, j):
        ins = [list(source) for source in zip(*sent)]
        whole_z = direct(j)
        mats = m_direct if whole_z else m_pair
        first_id = G if whole_z else 2 * G
        got = z_call((chained(mats[0]), mats[1]), ids, first_id, ins, 1 if whole_z else 2, half)
        mark(got[-1])
        if whole_z:
            return [got[0]]
        return [got[0], lax.ppermute(got[1], "yz", cross)]

    ghost = {}
    sends, parts, faces, solved = {}, {}, {}, {}
    meta = jnp.stack([offset, first.astype(jnp.int32), last.astype(jnp.int32)])

    def vel_halo(n, lo, hi):
        v = chained(vel)
        ghost[n] = (
            lax.ppermute(v[lo:hi, X - 3 :], "gx", ring("gx", 1)),
            lax.ppermute(v[lo:hi, :3], "gx", ring("gx", -1)),
        )

    def shear(n):
        ghost[n] = shear_call(chained(meta), *ghost[n])
        mark(*ghost[n])

    def spectra(i, *jobs, us=8):
        widths = widths_of(jobs[0][0])
        flat = spectra_call(
            i, [want for _, want in jobs], vel, ghost, ids, chained(background), omega,
            [f_pairs[j] + (kys[j],) for j, _ in jobs], widths, half, us,
        )
        mark(flat[-1])
        n = len(widths)
        for at, (j, _) in enumerate(jobs):
            sends.setdefault((i, j), []).append(scatter(flat[at * n : (at + 1) * n], j))

    def forward_z(i, j):
        parts[i, j] = gather_z(sends[i, j], j)

    p_halo = []

    def vectors(j):
        own = modes_of(g[None], j)
        ky = twice(unit_y * own.astype(f32))
        edge = unit_y * ((own * offset % NY).astype(f32) + fraction * own.astype(f32))
        ec, es = twice(jnp.cos(edge)), twice(jnp.sin(edge))
        vec = jnp.concatenate(
            [
                ky,
                jnp.where(first, ec, 1.0),
                jnp.where(first, es, 0.0),
                jnp.where(last, ec, 1.0),
                jnp.where(last, -es, 0.0),
                twice(jnp.where(own == 0, 1.0, 2.0).astype(f32)),
                jnp.zeros((2, wide), f32),
            ],
            axis=0,
        )
        return vec, 1.0 / (2.0 + ky * ky + kz * kz)

    def prep(j):
        vec, inv = vectors(j)
        mine = [parts[i, j] for i in range(3)]
        up, down = prep_call(mine, chained(vec), kz, half)
        mark(up, down)
        faces[j] = (
            vec,
            inv,
            mine,
            lax.ppermute(up, "gx", ring("gx", 1)),
            lax.ppermute(down, "gx", ring("gx", -1)),
        )

    def solve(j):
        vec, inv, mine, fl, fr = faces[j]
        q, p, groups = solve_call(
            j, half, G, ids, chained(vec), kz, inv, m_inv, mine, fl, fr,
            pressure_guess, p_halo[0], p_halo[1], q_old,
        )
        mark(q)
        solved[j] = (q, p, groups)

    def give_back(j):
        out = []
        for hs in solved[j][2]:
            got = [hs[0]]
            for s in range(1, G):
                got.append(lax.ppermute(hs[s], "yz", ring("yz", s)))
            out.append(got)
        return out

    def guess_halo():
        guess = chained(pressure_guess)
        p_halo.append(lax.ppermute(guess[X - 3 :], "gx", ring("gx", 1)))
        p_halo.append(lax.ppermute(guess[:3], "gx", ring("gx", -1)))

    if J == 2:
        spectra(0, (0, "uc"), us=6)
        vel_halo(0, 0, 1)
        vel_halo(1, 1, 3)
        spectra(1, (0, "uc"), us=6)
        shear(0)
        spectra(0, (0, "w"))
        spectra(2, (0, "uc"), us=6)
        shear(1)
        spectra(1, (0, "w"))
        spectra(2, (0, "w"))
        spectra(0, (1, "ucw"))
        spectra(1, (1, "ucw"))
        forward_z(0, 0)
        spectra(2, (1, "ucw"))
        guess_halo()
        forward_z(1, 0)
        forward_z(0, 1)
        forward_z(2, 0)
        prep(0)
        forward_z(1, 1)
        solve(0)
        forward_z(2, 1)
        prep(1)
        q, p, groups = solved[0]
        solved[0] = (q, p, [[chained(h) for h in hs] for hs in groups])
        got = give_back(0)
        solve(1)
        got1 = give_back(1)
        base = chained(vel)
        result = back_call(base, f_pairs[0], ids, got[0])
        result = back_call(result, f_pairs[1], ids, got1[0])
    else:
        if J > 2:
            raise NotImplementedError
        guess_halo()
        vel_halo(0, 0, 1)
        vel_halo(1, 1, 3)
        shear(0)
        shear(1)
        result = vel
        for j in range(J):
            for i in range(3):
                spectra(i, (j, "ucw"))
                forward_z(i, j)
            prep(j)
            solve(j)
            result = back_call(result, f_pairs[j], ids, give_back(j)[0])
    q_parts = [solved[j][0] for j in range(J)]
    p_parts = [solved[j][1] for j in range(J)]
    return result, pack_call(q_parts, half), pack_call(p_parts, half)


def solution(mesh):
    placed = (P(None, "gx", "yz", None), P(None, "gx", None, "yz"), P("gx", None, "yz"), P())
    return jax.shard_map(
        local,
        mesh=mesh,
        in_specs=placed,
        out_specs=(P(None, "gx", "yz", None), P(None, "gx", None, "yz"), P("gx", None, "yz")),
        check_vma=False,
    )
```

```python
import math

import jax
import jax.numpy as jnp
import numpy as np
from jax import lax
from jax.experimental import pallas as pl
from jax.experimental.pallas import tpu as pltpu
from jax.sharding import PartitionSpec as P


SWEEPS = 2
viscosity = 0.05
time_step = 0.2
keep_weight = -5.0 / 9.0
section_weight = 15.0 / 16.0
shear_param = 1.5
fraction = 0.375
f32 = jnp.float32
bf16 = jnp.bfloat16
COST_SCALE = 250_000_000


def params(mib, n=1):
    return pltpu.CompilerParams(
        vmem_limit_bytes=mib * 1024 * 1024, dimension_semantics=("arbitrary",) * n
    )


def cost(us):
    return pl.CostEstimate(flops=int(us * COST_SCALE), bytes_accessed=0, transcendentals=0)


def split_const(matrix):
    exact = matrix.astype(np.float32)
    high = exact.astype(jnp.bfloat16)
    low = (exact - high.astype(np.float32)).astype(jnp.bfloat16)
    return jnp.asarray(high), jnp.asarray(low)


def split_value(value):
    high = value.astype(bf16)
    return high, (value - high.astype(f32)).astype(bf16)


def dot3(a, b, contract=((1,), (0,))):
    dims = (contract, ((), ()))

    def one(x, y):
        return lax.dot_general(x, y, dims, preferred_element_type=f32)

    return one(a[0], b[0]) + one(a[0], b[1]) + one(a[1], b[0])


def full_spec(shape):
    zeros = (0,) * len(shape)
    return pl.BlockSpec(shape, lambda *_: zeros)


def lane_sign(half):
    lanes = lax.broadcasted_iota(jnp.int32, (1, 2 * half), 1)
    return jnp.where(lanes < half, -1.0, 1.0).astype(f32)


def rot(value, half):
    return pltpu.roll(value, half, axis=1) * lane_sign(half)


def y_matrix(width_y, modes):
    angle = 2.0 * np.pi / width_y * (np.arange(width_y)[:, None, None] * modes[None] % width_y)
    full = np.concatenate([np.cos(angle), -np.sin(angle)], axis=2)
    return split_const(full.reshape(width_y, -1) / math.sqrt(width_y))


def z_forward_matrix(depth, rows, sources):
    m = np.arange(depth)
    kz = (2.0 * np.pi / depth * np.where(m < depth // 2, m, m - depth))[:, None]
    blocks = []
    for source in sources:
        z = source * rows + np.arange(rows)
        wave = np.exp(-2j * np.pi / depth * (m[:, None] * z[None, :] % depth))
        blocks += [-viscosity * kz * kz * wave, 1j * kz * wave, wave]
    full = np.concatenate(blocks, axis=1) / math.sqrt(depth)
    return np.concatenate([full.real, full.imag], axis=0)


def z_inverse_matrix(depth):
    m = np.arange(depth)
    full = np.exp(2j * np.pi / depth * (m[:, None] * m[None, :] % depth)) / math.sqrt(depth)
    return split_const(np.concatenate([full.real, full.imag], axis=0))


def block_at(index, size):
    return pl.ds(pl.multiple_of(index * size, size), size)


def spectra_body(comp, omega, half, jobs, comps, n_out, ids, bg_ref, *rest):
    vels = dict(zip(comps, rest))
    rest = rest[len(comps) :]
    ui, u0, u1, u2 = vels[comp], vels.get(0), vels.get(1), vels.get(2)
    has_w = any("w" in want for want in jobs)
    has_c = any("c" in want for want in jobs)
    if has_w:
        n_h = 2 if comp == 0 else 4
        halos, rest = rest[:n_h], rest[n_h:]
    mats, rest = rest[: 3 * len(jobs)], rest[3 * len(jobs) :]
    outs, (buf, res) = rest[:-2], rest[-2:]
    _, X, Rz, NY = ui.shape
    d1 = (0.0, 45.0 / 60.0, -9.0 / 60.0, 1.0 / 60.0)
    d2 = (-490.0 / 180.0, 270.0 / 180.0, -27.0 / 180.0, 2.0 / 180.0)
    step = min(512, NY)
    base = 1 if has_c else 0

    def pick(i, at, rows, cols):
        if 0 <= at < X:
            return vels[i][0, at, rows, cols]
        ref = halos[(0 if i == 0 else 2) + (0 if at < 0 else 1)]
        return ref[0, at + 3 if at < 0 else at - X, rows, cols]

    def tile(r, carry):
        rows = pl.ds(pl.multiple_of(r // (NY // step) * 8, 8), 8)
        cols = pl.ds(pl.multiple_of(r % (NY // step) * step, step), step)
        for x in range(X):
            u = ui[0, x, rows, cols]
            if has_c:
                buf[0, x, rows, cols] = -u2[0, x, rows, cols] * u
            buf[base, x, rows, cols] = u
            if has_w:
                acc = (viscosity * d2[0]) * u
                for o in (1, 2, 3):
                    up = pick(comp, x + o, rows, cols)
                    dn = pick(comp, x - o, rows, cols)
                    if comp == 0:
                        xp, xm = up, dn
                    else:
                        xp = pick(0, x + o, rows, cols)
                        xm = pick(0, x - o, rows, cols)
                    acc = acc + (viscosity * d2[o]) * (up + dn)
                    acc = acc - d1[o] * (xp * up - xm * dn)
                if comp == 0:
                    acc = acc + (2.0 * omega) * u1[0, x, rows, cols]
                if comp == 1:
                    acc = acc - ((2.0 - shear_param) * omega) * u0[0, x, rows, cols]
                buf[base + 1, x, rows, cols] = acc
                buf[base + 2, x, rows, cols] = -(u1[0, x, rows, cols] + bg_ref[x]) * u
        return carry

    lax.fori_loop(0, Rz // 8 * (NY // step), tile, 0)
    M = X * Rz
    wide = 2 * half
    for n, want in enumerate(jobs):
        lo = 0 if "c" in want else base
        hi = base + (3 if "w" in want else 1)
        high, low, vec_ref = mats[3 * n : 3 * n + 3]

        def product(f, carry):
            lhs = split_value(buf[f].reshape(M, NY))
            res[f] = dot3(lhs, (high[...], low[...]))
            return carry

        lax.fori_loop(lo, hi, product, 0)
        slot = 0
        for out in outs[n * n_out : (n + 1) * n_out]:
            for j in range(out.shape[-1] // wide):
                cols = block_at(ids[slot], wide)
                own = slice(j * wide, (j + 1) * wide)
                yu = res[base, :, cols]
                if "c" in want:
                    out[0, :, :, own] = yu.reshape(X, Rz, wide)
                    out[1, :, :, own] = res[0, :, cols].reshape(X, Rz, wide)
                if "w" in want:
                    ky = vec_ref[0:1, cols]
                    w = (
                        res[base + 1, :, cols]
                        + ky * rot(res[base + 2, :, cols], half)
                        - (viscosity * ky * ky) * yu
                    )
                    out[len(want) - 1, :, :, own] = w.reshape(X, Rz, wide)
                slot += 1


def spectra_call(comp, jobs, vel, ghost, ids, background, omega, mats, widths, half, us):
    _, X, Rz, NY = vel.shape
    has_w = any("w" in want for want in jobs)
    has_c = any("c" in want for want in jobs)
    comps = sorted({comp} | ({2} if has_c else set()) | ({0, 1} if has_w else set()))
    plane = lambda i: pl.BlockSpec((1, X, Rz, NY), lambda *_: (i, 0, 0, 0))
    halos, halo_specs = [], []
    if has_w:
        halos = list(ghost[0]) + (list(ghost[1]) if comp else [])
        block = (1,) + halos[0].shape[1:]
        halo_specs = [pl.BlockSpec(block, lambda *_: (0, 0, 0, 0))] * 2
        if comp:
            halo_specs += [pl.BlockSpec(block, lambda *_: (comp - 1, 0, 0, 0))] * 2
    count = (2 if has_c else 1) + (2 if has_w else 0)
    flat = [a for m in mats for a in m]
    shapes = [(len(want), X, Rz, w) for want in jobs for w in widths]
    return pl.pallas_call(
        lambda *refs: spectra_body(comp, omega, half, jobs, comps, len(widths), *refs),
        grid=(1,),
        in_specs=[pl.BlockSpec(memory_space=pltpu.SMEM)] * 2
        + [plane(c) for c in comps]
        + halo_specs
        + [full_spec(a.shape) for a in flat],
        out_specs=[full_spec(shape) for shape in shapes],
        out_shape=[jax.ShapeDtypeStruct(shape, f32) for shape in shapes],
        scratch_shapes=[
            pltpu.VMEM((count, X, Rz, NY), f32),
            pltpu.VMEM((count, X * Rz, sum(widths)), f32),
        ],
        compiler_params=params(50),
        cost_estimate=cost(us),
        name="spectra",
    )(ids, background, *([vel] * len(comps)), *halos, *flat)


def z_body(counts, first_id, n_t, half, ids, mh_ref, ml_ref, *rest):
    n_in = len(counts)
    ins, outs, buf = rest[:n_in], rest[n_in : n_in + n_t], rest[-1]
    _, X, Rz, _ = ins[0].shape
    wide = 2 * half
    depth = outs[0].shape[1]
    for t in range(n_t):
        own = slice(t * wide, (t + 1) * wide)
        n = 0
        for ref, count in zip(ins, counts):
            for f in range(count):
                rows = block_at(ids[first_id + n // 3] * 3 + n % 3, Rz)
                for x in range(X):
                    col = (t * X + x) * wide
                    buf[rows, col : col + wide] = ref[f, x, :, own]
                n += 1
    res = dot3((mh_ref[...], ml_ref[...]), split_value(buf[...]))
    for t in range(n_t):
        for x in range(X):
            col = (t * X + x) * wide
            cols = slice(col, col + wide)
            outs[t][x] = res[:depth, cols] + rot(res[depth:, cols], half)


def z_call(m_pair, ids, first_id, ins, n_t, half):
    flat = [a for source in ins for a in source]
    counts = [a.shape[0] for a in flat]
    _, X, Rz, _ = flat[0].shape
    depth = m_pair[0].shape[0] // 2
    return pl.pallas_call(
        lambda *refs: z_body(counts, first_id, n_t, half, *refs),
        in_specs=[pl.BlockSpec(memory_space=pltpu.SMEM)]
        + [pl.BlockSpec(memory_space=pltpu.VMEM)] * (2 + len(flat)),
        out_shape=[jax.ShapeDtypeStruct((X, depth, 2 * half), f32)] * n_t,
        scratch_shapes=[pltpu.VMEM((sum(counts) * Rz, n_t * X * 2 * half), f32)],
        compiler_params=params(24, 0),
        cost_estimate=cost(4),
        name="zforward",
    )(ids, *m_pair, *flat)


def shear_body(meta, up, down, up_out, down_out):
    NY = up.shape[-1]
    shift = meta[0]

    def one(flag, ref, out, by, by_next):
        @pl.when(flag == 1)
        def _():
            v = ref[0, 0]
            out[0, 0] = (1.0 - fraction) * pltpu.roll(v, by, 1) + fraction * pltpu.roll(v, by_next, 1)

        @pl.when(flag == 0)
        def _():
            out[0, 0] = ref[0, 0]

    one(meta[1], up, up_out, (NY - shift) % NY, (2 * NY - shift - 1) % NY)
    one(meta[2], down, down_out, shift % NY, (shift + 1) % NY)


def shear_call(meta, up, down):
    n, w, Rz, NY = up.shape
    spec = pl.BlockSpec((1, 1, Rz, NY), lambda i, x: (i, x, 0, 0))
    return pl.pallas_call(
        shear_body,
        grid=(n, w),
        in_specs=[pl.BlockSpec(memory_space=pltpu.SMEM), spec, spec],
        out_specs=[spec, spec],
        out_shape=[jax.ShapeDtypeStruct(up.shape, f32)] * 2,
        compiler_params=params(16, 2),
        cost_estimate=cost(3),
        name="shear",
    )(meta, up, down)


def blocks_of(depth):
    return 4 if depth % 32 == 0 else 1


def row_block(lead, rows, wide):
    zeros = (0,) * len(lead)
    return pl.BlockSpec(tuple(lead) + (rows, wide), lambda b: zeros + (b, 0))


def add_parts(parts, x, rows):
    v = parts[0][x, rows]
    for p in parts[1:]:
        v = v + p[x, rows]
    return v


def cut(refs, counts):
    out, at = [], 0
    for n in counts:
        out.append(refs[at : at + n])
        at += n
    return out, refs[at:]


def prep_body(counts, half, vec_ref, kz_ref, *rest):
    parts, (up, down) = cut(rest, counts)
    X, depth = parts[0][0].shape[:2]
    ky = vec_ref[0:1]

    def tile(r, carry):
        rows = pl.ds(pl.multiple_of(r * 8, 8), 8)
        kz = kz_ref[rows]
        for x in range(X):
            if x < 3 or x >= X - 3:
                t = add_parts(parts[0], x, rows)
                if x < 3:
                    down[x, rows] = t
                if x >= X - 3:
                    up[x - X + 3, rows] = t
            if x < 2 or x >= X - 2:
                d = rot(ky * add_parts(parts[1], x, rows) + kz * add_parts(parts[2], x, rows), half)
                if x < 2:
                    down[3 + x, rows] = d
                if x >= X - 2:
                    up[3 + x - X + 2, rows] = d
        return carry

    lax.fori_loop(0, depth // 8, tile, 0)


def prep_call(parts, vec, kz, half):
    X, depth, wide = parts[0][0].shape
    n = [len(p) for p in parts]
    nb = blocks_of(depth)
    rows = depth // nb
    flat = [a for p in parts for a in p]
    return pl.pallas_call(
        lambda *refs: prep_body(n, half, *refs),
        grid=(nb,),
        in_specs=[full_spec(vec.shape), row_block((), rows, wide)]
        + [row_block((X,), rows, wide)] * len(flat),
        out_specs=[row_block((5,), rows, wide)] * 2,
        out_shape=[jax.ShapeDtypeStruct((5, depth, wide), f32)] * 2,
        compiler_params=params(24),
        cost_estimate=cost(4),
        name="prep",
    )(vec, kz, *flat)


def take_chunk(ref, lead, rows, chunk, half):
    total = ref.shape[-1]
    if total == 2 * half:
        return ref[lead + (rows,)]
    wide = 2 * half
    assert total == 2 * wide
    re = ref[lead + (rows, slice(0, wide))]
    im = ref[lead + (rows, slice(wide, total))]
    low = lax.broadcasted_iota(jnp.int32, (1, wide), 1) < half
    if chunk == 0:
        return jnp.where(low, re, pltpu.roll(im, half, axis=1))
    return jnp.where(low, pltpu.roll(re, half, axis=1), im)


def solve_body(chunk, half, n_slot, counts, nb, ids, vec_ref, kz_ref, inv_ref, mh_ref, ml_ref, fl, fr, p0, p0l, p0r, q_old, *rest):
    parts, rest = cut(rest, counts)
    q_out, p_out = rest[:2]
    outs, buf = rest[2:-1], rest[-1]
    X, depth = p_out.shape[:2]
    wide = 2 * half
    ky = vec_ref[0:1]
    cl, sl = vec_ref[1:2], vec_ref[2:3]
    cr, sr = vec_ref[3:4], vec_ref[4:5]
    step = pl.program_id(0)

    def left(v):
        return v * cl + rot(v, half) * sl

    def right(v):
        return v * cr + rot(v, half) * sr

    def tile(r, carry):
        rows = pl.ds(pl.multiple_of(r * 8, 8), 8)
        whole = pl.ds(pl.multiple_of(step * depth + r * 8, 8), 8)
        kz = kz_ref[rows]
        inv = inv_ref[rows]
        tx, ty, tz, dd, pp = {}, {}, {}, {}, {}
        for x in range(X):
            tx[x] = add_parts(parts[0], x, rows)
            ty[x] = add_parts(parts[1], x, rows)
            tz[x] = add_parts(parts[2], x, rows)
            dd[x] = rot(ky * ty[x] + kz * tz[x], half)
            pp[x] = take_chunk(p0, (x,), rows, chunk, half)
        for o in range(3):
            tx[o - 3] = left(fl[o, rows])
            tx[X + o] = right(fr[o, rows])
            pp[o - 3] = left(take_chunk(p0l, (o,), rows, chunk, half))
            pp[X + o] = right(take_chunk(p0r, (o,), rows, chunk, half))
        for o in range(2):
            dd[o - 2] = left(fl[3 + o, rows])
            dd[X + o] = right(fr[3 + o, rows])
        div = {x: 0.5 * (tx[x + 1] - tx[x - 1]) + dd[x] for x in range(-2, X + 2)}
        for sweep in range(SWEEPS):
            reach = SWEEPS - sweep
            pp = {
                x: (pp[x + 1] + pp[x - 1] - div[x]) * inv
                for x in range(-reach, X + reach)
            }
        for x in range(X):
            p = pp[x]
            p_out[x, rows] = p
            ip = rot(p, half)
            grad = (0.5 * (pp[x + 1] - pp[x - 1]), ky * ip, kz * ip)
            for i, now in enumerate((tx[x], ty[x], tz[x])):
                old = take_chunk(q_old, (i, x), rows, chunk, half)
                q = keep_weight * old + time_step * (now - grad[i])
                q_out[i, x, rows] = q
                buf[i, whole, x * wide : (x + 1) * wide] = q
        return carry

    lax.fori_loop(0, depth // 8, tile, 0)

    @pl.when(step == nb - 1)
    def _():
        total = depth * nb
        Rz = total // n_slot
        mats = (mh_ref[...], ml_ref[...])
        for i in range(3):
            res = dot3(mats, split_value(buf[i]))
            for x in range(X):
                cols = slice(x * wide, (x + 1) * wide)
                buf[i, :, cols] = (res[:total, cols] + rot(res[total:, cols], half)) * vec_ref[5:6]
            for s in range(n_slot):
                rows = block_at(ids[2 * n_slot + 2 + s], Rz)
                for x in range(X):
                    outs[s][i, x] = buf[i, rows, x * wide : (x + 1) * wide]


def solve_call(chunk, half, n_slot, ids, vec, kz, inv, m_pair, parts, fl, fr, p0, p0l, p0r, q_old):
    X, depth, wide = parts[0][0].shape
    nb = blocks_of(depth)
    rows = depth // nb
    n = [len(p) for p in parts]
    flat = [a for p in parts for a in p]
    packed = p0.shape[-1]
    n_h = n_slot
    h_shape = (3, X, depth // n_slot, wide)
    out = pl.pallas_call(
        lambda *refs: solve_body(chunk, half, n_slot, n, nb, *refs),
        grid=(nb,),
        in_specs=[
            pl.BlockSpec(memory_space=pltpu.SMEM),
            full_spec(vec.shape),
            row_block((), rows, wide),
            row_block((), rows, wide),
            full_spec(m_pair[0].shape),
            full_spec(m_pair[1].shape),
            row_block((5,), rows, wide),
            row_block((5,), rows, wide),
            row_block((X,), rows, packed),
            row_block((3,), rows, packed),
            row_block((3,), rows, packed),
            row_block((3, X), rows, packed),
        ]
        + [row_block((X,), rows, wide)] * len(flat),
        out_specs=[row_block((3, X), rows, wide), row_block((X,), rows, wide)]
        + [full_spec(h_shape)] * n_h,
        out_shape=[
            jax.ShapeDtypeStruct((3, X, depth, wide), f32),
            jax.ShapeDtypeStruct((X, depth, wide), f32),
        ]
        + [jax.ShapeDtypeStruct(h_shape, f32)] * n_h,
        scratch_shapes=[pltpu.VMEM((3, depth, X * wide), f32)],
        compiler_params=params(40),
        cost_estimate=cost(10),
        name="solve",
    )(ids, vec, kz, inv, *m_pair, fl, fr, p0, p0l, p0r, q_old, *flat)
    return out[0], out[1], [list(out[2:])]


def back_body(n_slot, ids, base_ref, gh_ref, gl_ref, *rest):
    hs, (out, buf) = rest[:n_slot], rest[n_slot:]
    _, X, Rz, wide = hs[0].shape
    for s, h in enumerate(hs):
        buf[:, block_at(ids[3 * n_slot + 2 + s], wide)] = h[...].reshape(X * Rz, wide)
    res = dot3(split_value(buf[...]), (gh_ref[...], gl_ref[...]), ((1,), (1,)))
    out[...] = base_ref[...] + section_weight * res.reshape(out.shape)


def back_call(base, g_pair, ids, hs):
    _, X, Rz, NY = base.shape
    wide = hs[0].shape[-1]
    plane = lambda w: pl.BlockSpec((1, X, Rz, w), lambda i: (i, 0, 0, 0))
    return pl.pallas_call(
        lambda *refs: back_body(len(hs), *refs),
        grid=(3,),
        in_specs=[
            pl.BlockSpec(memory_space=pltpu.SMEM),
            plane(NY),
            full_spec(g_pair[0].shape),
            full_spec(g_pair[1].shape),
        ]
        + [plane(wide)] * len(hs),
        out_specs=plane(NY),
        out_shape=jax.ShapeDtypeStruct(base.shape, f32),
        scratch_shapes=[pltpu.VMEM((X * Rz, len(hs) * wide), f32)],
        compiler_params=params(32),
        cost_estimate=cost(7),
        name="back",
    )(ids, base, *g_pair, *hs)


def pack_body(half, a_ref, b_ref, out):
    wide = 2 * half
    low = lax.broadcasted_iota(jnp.int32, (1, wide), 1) < half
    for n in range(a_ref.shape[0]):
        a, b = a_ref[n], b_ref[n]
        out[n, :, 0:wide] = jnp.where(low, a, pltpu.roll(b, half, axis=1))
        out[n, :, wide : 2 * wide] = jnp.where(low, pltpu.roll(a, half, axis=1), b)


def pack_call(chunks, half):
    if len(chunks) == 1:
        return chunks[0]
    a, b = chunks
    lead, (depth, wide) = a.shape[:-2], a.shape[-2:]
    n = math.prod(lead)
    per = 3 if n % 3 == 0 else 1
    spec = lambda w: pl.BlockSpec((per, depth, w), lambda i: (i, 0, 0))
    out = pl.pallas_call(
        lambda *refs: pack_body(half, *refs),
        grid=(n // per,),
        in_specs=[spec(wide), spec(wide)],
        out_specs=spec(2 * wide),
        out_shape=jax.ShapeDtypeStruct((n, depth, 2 * wide), f32),
        compiler_params=params(16),
        cost_estimate=cost(5),
        name="pack",
    )(a.reshape(n, depth, wide), b.reshape(n, depth, wide))
    return out.reshape(lead + (depth, 2 * wide))


def ring(axis, shift):
    count = lax.axis_size(axis)
    return [(i, (i + shift) % count) for i in range(count)]


def after(value, *deps):
    return lax.optimization_barrier((value,) + deps)[0]


def local(vel, q_old, pressure_guess, shear_shift):
    X, Rz, NY = vel.shape[1:]
    depth = q_old.shape[2]
    G = lax.axis_size("yz")
    L = NY // (2 * G)
    half = 64 if L % 64 == 0 else L
    J = L // half
    wide = 2 * half
    g = lax.axis_index("yz")
    slab = lax.axis_index("gx")
    slabs = lax.axis_size("gx")
    total_x = X * slabs
    offset = shear_shift[0]
    omega = 2.0 / total_x
    paired = G == 4
    first, last = slab == 0, slab == slabs - 1

    if paired:
        slot_groups = jnp.stack([g, G - 1 - g, g ^ 1, G - 1 - (g ^ 1)])
        slot_sources = slot_groups
    else:
        slot_groups = (g + jnp.arange(G, dtype=jnp.int32)) % G
        slot_sources = (g - jnp.arange(G, dtype=jnp.int32)) % G
    back_groups = (g - jnp.arange(G, dtype=jnp.int32)) % G

    def modes_of(groups, j):
        return groups[:, None] * L + j * half + jnp.arange(half, dtype=jnp.int32)[None, :]

    unit_y = 2.0 * math.pi / NY

    def twice(a):
        return jnp.concatenate([a, a], axis=-1).reshape(1, -1)

    m = jnp.arange(depth, dtype=jnp.int32)
    signed = jnp.where(m < depth // 2, m, m - depth)
    kz1 = 2.0 * math.pi / depth * signed.astype(f32)
    kz = jnp.broadcast_to(kz1[:, None], (depth, wide))
    m_inv = z_inverse_matrix(depth)
    m_direct = split_const(z_forward_matrix(depth, Rz, range(G)))
    pair_at = jnp.stack([g % 2, 1 - g % 2])
    if paired:
        halves = [split_const(z_forward_matrix(depth, Rz, (n, n + 1))) for n in (0, 2)]
        m_pair = [jnp.where(g < 2, low, high) for low, high in zip(*halves)]
    dest = (g + jnp.arange(G, dtype=jnp.int32)) % G
    ids = jnp.concatenate([slot_groups, slot_sources, pair_at, dest, back_groups])
    xpos = (slab * X + jnp.arange(X, dtype=jnp.int32)).astype(f32) + 0.5 - total_x / 2.0
    background = -shear_param * omega * xpos

    f_pairs, kys = [], []
    for j in range(J):
        modes = np.arange(G)[:, None] * L + j * half + np.arange(half)[None, :]
        f_pairs.append(y_matrix(NY, modes))
        both = np.concatenate([modes, modes], axis=1).reshape(1, -1)
        kys.append(jnp.asarray((unit_y * both).astype(np.float32)))

    swap = [(i, i ^ 1) for i in range(G)]
    cross = [(i, G - 1 - i) for i in range(G)]
    if paired:
        slot_perms = [None, cross, swap, ring("yz", 2)]
    else:
        slot_perms = [ring("yz", s) for s in range(G)]

    def direct(i, j):
        return not paired or (i, j) in ((0, 0), (2, 0), (2, 1))

    def widths_of(i, j):
        return [wide] * G if direct(i, j) else [2 * wide] * 2

    def scatter(pieces, i, j):
        perms = slot_perms if direct(i, j) else [None, swap]
        order = [2, 3, 1] if paired and direct(i, j) else range(1, len(pieces))
        out = [pieces[0]] + [None] * (len(pieces) - 1)
        for s in order:
            out[s] = lax.ppermute(pieces[s], "yz", perms[s])
        return out

    token = []

    def chained(value):
        return after(value, *token) if token else value

    def mark(*arrays):
        token[:] = arrays

    def gather_z(sent, i, j):
        ins = [list(source) for source in zip(*sent)]
        whole_z = direct(i, j)
        mats = m_direct if whole_z else m_pair
        first_id = G if whole_z else 2 * G
        got = z_call((chained(mats[0]), mats[1]), ids, first_id, ins, 1 if whole_z else 2, half)
        mark(got[-1])
        if whole_z:
            return [got[0]]
        return [got[0], lax.ppermute(got[1], "yz", cross)]

    ghost = {}
    sends, parts, faces, solved = {}, {}, {}, {}
    meta = jnp.stack([offset, first.astype(jnp.int32), last.astype(jnp.int32)])

    def vel_halo(n, lo, hi):
        v = chained(vel)
        ghost[n] = (
            lax.ppermute(v[lo:hi, X - 3 :], "gx", ring("gx", 1)),
            lax.ppermute(v[lo:hi, :3], "gx", ring("gx", -1)),
        )

    def shear(n):
        ghost[n] = shear_call(chained(meta), *ghost[n])
        mark(*ghost[n])

    def spectra(i, *jobs, us=8):
        widths = widths_of(i, jobs[0][0])
        flat = spectra_call(
            i, [want for _, want in jobs], vel, ghost, ids, chained(background), omega,
            [f_pairs[j] + (kys[j],) for j, _ in jobs], widths, half, us,
        )
        mark(flat[-1])
        n = len(widths)
        for at, (j, _) in enumerate(jobs):
            sends.setdefault((i, j), []).append(scatter(flat[at * n : (at + 1) * n], i, j))

    def forward_z(i, j):
        parts[i, j] = gather_z(sends[i, j], i, j)

    p_halo = []

    def vectors(j):
        own = modes_of(g[None], j)
        ky = twice(unit_y * own.astype(f32))
        edge = unit_y * ((own * offset % NY).astype(f32) + fraction * own.astype(f32))
        ec, es = twice(jnp.cos(edge)), twice(jnp.sin(edge))
        vec = jnp.concatenate(
            [
                ky,
                jnp.where(first, ec, 1.0),
                jnp.where(first, es, 0.0),
                jnp.where(last, ec, 1.0),
                jnp.where(last, -es, 0.0),
                twice(jnp.where(own == 0, 1.0, 2.0).astype(f32)),
                jnp.zeros((2, wide), f32),
            ],
            axis=0,
        )
        return vec, 1.0 / (2.0 + ky * ky + kz * kz)

    def prep(j):
        vec, inv = vectors(j)
        mine = [parts[i, j] for i in range(3)]
        up, down = prep_call(mine, chained(vec), kz, half)
        mark(up, down)
        faces[j] = (
            vec,
            inv,
            mine,
            lax.ppermute(up, "gx", ring("gx", 1)),
            lax.ppermute(down, "gx", ring("gx", -1)),
        )

    def solve(j):
        vec, inv, mine, fl, fr = faces[j]
        q, p, groups = solve_call(
            j, half, G, ids, chained(vec), kz, inv, m_inv, mine, fl, fr,
            pressure_guess, p_halo[0], p_halo[1], q_old,
        )
        mark(q)
        solved[j] = (q, p, groups)

    def give_back(j):
        out = []
        for hs in solved[j][2]:
            got = [hs[0]]
            for s in range(1, G):
                got.append(lax.ppermute(hs[s], "yz", ring("yz", s)))
            out.append(got)
        return out

    def guess_halo():
        guess = chained(pressure_guess)
        p_halo.append(lax.ppermute(guess[X - 3 :], "gx", ring("gx", 1)))
        p_halo.append(lax.ppermute(guess[:3], "gx", ring("gx", -1)))

    if J == 2:
        spectra(0, (0, "uc"), us=6)
        vel_halo(0, 0, 1)
        vel_halo(1, 1, 3)
        spectra(1, (0, "uc"), us=6)
        shear(0)
        spectra(0, (0, "w"))
        spectra(2, (0, "uc"), us=6)
        shear(1)
        spectra(1, (0, "w"))
        spectra(2, (0, "w"))
        spectra(0, (1, "ucw"))
        forward_z(1, 0)
        spectra(1, (1, "ucw"))
        forward_z(0, 0)
        spectra(2, (1, "ucw"))
        guess_halo()
        forward_z(0, 1)
        forward_z(2, 0)
        prep(0)
        forward_z(1, 1)
        solve(0)
        forward_z(2, 1)
        q, p, groups = solved[0]
        arrived = parts[0, 1][1:] + parts[1, 1][1:]
        solved[0] = (q, p, [[after(chained(h), *arrived) for h in hs] for hs in groups])
        got = give_back(0)
        prep(1)
        solve(1)
        got1 = give_back(1)
        base = chained(vel)
        result = back_call(base, f_pairs[0], ids, got[0])
        result = back_call(result, f_pairs[1], ids, got1[0])
    else:
        if J > 2:
            raise NotImplementedError
        guess_halo()
        vel_halo(0, 0, 1)
        vel_halo(1, 1, 3)
        shear(0)
        shear(1)
        result = vel
        for j in range(J):
            for i in range(3):
                spectra(i, (j, "ucw"))
                forward_z(i, j)
            prep(j)
            solve(j)
            result = back_call(result, f_pairs[j], ids, give_back(j)[0])
    q_parts = [solved[j][0] for j in range(J)]
    p_parts = [solved[j][1] for j in range(J)]
    return result, pack_call(q_parts, half), pack_call(p_parts, half)


def solution(mesh):
    placed = (P(None, "gx", "yz", None), P(None, "gx", None, "yz"), P("gx", None, "yz"), P())
    return jax.shard_map(
        local,
        mesh=mesh,
        in_specs=placed,
        out_specs=(P(None, "gx", "yz", None), P(None, "gx", None, "yz"), P("gx", None, "yz")),
        check_vma=False,
    )
```
